32 devices in a mesh: gx: 4 (over x, core), gy: 4 (over z), gz: 2 (over y).
Axes of the slice: x: 2, y: 2, z: 4, core: 2. Of those that a mesh axis runs over, the one named last changes fastest.
Arguments:
- chemical_log_concentrations: float32 [53, 12, 96, 256], P(None, 'gx', 'gy', 'gz'), may hold values from -6 to 6
- advection_wind: float32 [3, 12, 96, 256], P(None, 'gx', 'gy', 'gz'), may hold values from -1 to 1
- inverse_thermal_scale: float32 [12, 96, 256], P('gx', 'gy', 'gz'), may hold values from 0.3 to 1.2
- kinetics_column_switch: int32 [1, 12, 96, 2], P(None, 'gx', 'gy', 'gz'), may hold values from 0 to 1, as said below
- kinetic_exponents: bfloat16 [192, 53], replicated, may hold values from -0.875 to 0.875
- arrhenius_log_coefficient: float32 [192], replicated, may hold values from -2 to 0
- arrhenius_energy: float32 [192], replicated, may hold values from 0.5 to 4
- stoichiometric_production: bfloat16 [53, 192], replicated, may hold values from -0.4375 to 0.4375
- formation_heat: float32 [53], replicated, may hold values from -0.875 to 0.875
- streamwise_tucker_basis: float32 [12, 64], P('gx'), may hold values from -1.75 to 1.75
Outputs:
- species_out: float32 [53, 12, 96, 256], P(None, 'gx', 'gy', 'gz')
- core: float32 [4, 64, 24, 256], P('gy', None, 'gx', 'gz')
The draws below stay inside these ranges and needn't reach their ends.
Inputs may be any that keep to these rules, and one draw needn't show every extreme that they name: `kinetics_column_switch`: A pencil is the 128 cells along z of one device at one x and y. In each evaluation the 8 devices that share an index of gx hold exactly 128 hot pencils together, no device holds more than 64, and one of them holds exactly 64.
All inputs are finite; a program needn't handle non-finite values.
Results may differ from the reference program's by a relative error of at most 0.0065.
Values may be sent and summed in bfloat16 or wider, within the bound.
No kernel may reach another device: no remote copies, remote signals or barrier semaphores. Data moves between devices by JAX's collectives and lax.ppermute only.
A program may use at most 128 MiB of HBM per device.

```python
import math
import jax
import jax.numpy as jnp
from jax import lax

SPECIES = 53
REACTIONS = 192
MODES = 64
CHEMISTRY_CALLS = 1
SUBSTEPS = 2
CX = 3
CY = 24
COLUMN_DEPTH = 128
LOAD = 16
MOST = 64
GRID_WIDTH_EAST = 12
GRID_WIDTH_NORTH = 96
GRID_WIDTH_UPWARD = 256
COLUMN_TALLY = 2
N_GX = 4
N_GY = 4
N_GZ = 2


def draw_kinetics_column_switch(key, part):
    stream = jax.random.fold_in(key, 7117)
    x_block_count = GRID_WIDTH_EAST // CX
    blocks_y = GRID_WIDTH_NORTH // CY
    blocks_z = GRID_WIDTH_UPWARD // COLUMN_DEPTH
    member_list = blocks_y * blocks_z
    columns = CX * CY
    overall_cell_count = member_list * columns
    chosen_count = LOAD * member_list
    first_key, secondary_key, third_key, fourth_key = jax.random.split(stream, 4)
    shape_full = (CHEMISTRY_CALLS, x_block_count, member_list, columns)
    order_score = jax.random.randint(fourth_key, shape_full, 0, 65536) * columns + jnp.arange(columns).reshape(1, 1, 1, columns)
    within_rank = jnp.argsort(jnp.argsort(order_score, axis=-1), axis=-1)
    proposal_entry = within_rank < MOST
    baseline_rating = jax.random.randint(first_key, shape_full, 0, 256)
    device_reward = jax.random.randint(secondary_key, (CHEMISTRY_CALLS, x_block_count, member_list, 1), 0, 3) * 100
    leader = jax.random.randint(third_key, (CHEMISTRY_CALLS, x_block_count, 1, 1), 0, member_list)
    compelled_flag = jnp.where(jnp.arange(member_list).reshape(1, 1, member_list, 1) == leader, 2048, 0)
    rank_position = jnp.arange(overall_cell_count).reshape(1, 1, member_list, columns)
    rating_value = jnp.where(proposal_entry, (baseline_rating + device_reward + compelled_flag + 1) * overall_cell_count + rank_position, rank_position)
    rating_value = rating_value.reshape(CHEMISTRY_CALLS, x_block_count, overall_cell_count)
    picked = lax.top_k(rating_value, chosen_count)[1]

    def mark(indices):
        return jnp.zeros((overall_cell_count,), jnp.int32).at[indices].set(1)
    marked = jax.vmap(jax.vmap(mark))(picked)
    marked = marked.reshape(CHEMISTRY_CALLS, x_block_count, blocks_y, blocks_z, CX, CY)
    marked = marked.transpose(0, 1, 4, 2, 5, 3)
    return marked.reshape(CHEMISTRY_CALLS, GRID_WIDTH_EAST, GRID_WIDTH_NORTH, blocks_z)


def steps_of(rng, shape, pieces, least, high):
    factor_of = 1.0
    for axis_at, shards_of in pieces:
        steps = jax.random.uniform(jax.random.fold_in(jax.random.fold_in(rng, 6), axis_at), (shards_of,), jnp.float32, least / len(pieces), high / len(pieces))
        factor_of = factor_of * jnp.repeat(jnp.exp(steps), shape[axis_at] // shards_of).reshape((-1,) + (1,) * (len(shape) - 1 - axis_at))
    return factor_of


def noise(own_key, shape, deviation, bound, cuts=(), held_as=jnp.bfloat16):
    array = jax.random.normal(own_key, shape, jnp.float32) * deviation
    if len(cuts) > 0:
        array = steps_of(own_key, shape, cuts, -0.22, 0.18) * array
    return jnp.clip(array, min=-bound, max=bound).astype(held_as)


def setup_inputs(seed: int = 0) -> dict:
    key_of = jax.random.split(jax.random.key(seed), 11)
    return {
        "chemical_log_concentrations": noise(key_of[0], (SPECIES, GRID_WIDTH_EAST, GRID_WIDTH_NORTH, GRID_WIDTH_UPWARD), 1.0, 6.0, ((1, 4), (2, 4), (3, 2)), jnp.float32),
        "advection_wind": jnp.clip(jax.random.uniform(key_of[1], (3, GRID_WIDTH_EAST, GRID_WIDTH_NORTH, GRID_WIDTH_UPWARD), jnp.float32, -1.0, 1.0) * steps_of(key_of[1], (3, GRID_WIDTH_EAST, GRID_WIDTH_NORTH, GRID_WIDTH_UPWARD), ((1, 4), (2, 4), (3, 2)), -0.4, 0.0), -1.0, 1.0),
        "inverse_thermal_scale": jnp.clip(0.3 + 0.90000004 * jax.random.uniform(key_of[2], (GRID_WIDTH_EAST, GRID_WIDTH_NORTH, GRID_WIDTH_UPWARD), jnp.float32) ** steps_of(key_of[2], (GRID_WIDTH_EAST, GRID_WIDTH_NORTH, GRID_WIDTH_UPWARD), ((0, 4), (1, 4), (2, 2)), -0.2, 0.2), 0.3, 1.2),
        "kinetics_column_switch": draw_kinetics_column_switch(jax.random.fold_in(key_of[10], 71), 0),
        "kinetic_exponents": noise(key_of[4], (REACTIONS, SPECIES), SPECIES ** -0.5, 0.875),
        "arrhenius_log_coefficient": jnp.clip(jax.random.uniform(key_of[5], (REACTIONS,), jnp.float32, -2.0, 0.0), -2.0, 0.0),
        "arrhenius_energy": jnp.clip(jnp.exp(jax.random.uniform(key_of[6], (REACTIONS,), jnp.float32, math.log(0.5), math.log(4.0))), 0.5, 4.0),
        "stoichiometric_production": noise(key_of[7], (SPECIES, REACTIONS), REACTIONS ** -0.5, 0.4375),
        "formation_heat": noise(key_of[8], (SPECIES,), SPECIES ** -0.5, 0.875, (), jnp.float32),
        "streamwise_tucker_basis": noise(key_of[9], (GRID_WIDTH_EAST, MODES), GRID_WIDTH_EAST ** -0.5, 1.75, ((0, 4),), jnp.float32),
    }


flow_step = 0.15
sub_step = 0.04
smooth_eps = 1e-6


def reconstruct(first, second, middle, fourth, fifth):
    cand_zero = (2.0 * first - 7.0 * second + 11.0 * middle) / 6.0
    cand_one = (-second + 5.0 * middle + 2.0 * fourth) / 6.0
    cand_two = (2.0 * middle + 5.0 * fourth - fifth) / 6.0
    beta_zero = 13.0 / 12.0 * (first - 2.0 * second + middle) ** 2 + 0.25 * (first - 4.0 * second + 3.0 * middle) ** 2
    beta_one = 13.0 / 12.0 * (second - 2.0 * middle + fourth) ** 2 + 0.25 * (second - fourth) ** 2
    beta_two = 13.0 / 12.0 * (middle - 2.0 * fourth + fifth) ** 2 + 0.25 * (3.0 * middle - 4.0 * fourth + fifth) ** 2
    alpha_zero = 0.1 / (smooth_eps + beta_zero) ** 2
    alpha_one = 0.6 / (smooth_eps + beta_one) ** 2
    alpha_two = 0.3 / (smooth_eps + beta_two) ** 2
    return (alpha_zero * cand_zero + alpha_one * cand_one + alpha_two * cand_two) / (alpha_zero + alpha_one + alpha_two)


def upwind(padded, direction, extent, speed):
    def piece(start):
        return lax.slice_in_dim(padded, start, start + extent + 1, axis=direction)

    lower_faces = reconstruct(piece(0), piece(1), piece(2), piece(3), piece(4))
    upper_faces = reconstruct(piece(5), piece(4), piece(3), piece(2), piece(1))

    def differ(faces):
        return lax.slice_in_dim(faces, 1, extent + 1, axis=direction) - lax.slice_in_dim(faces, 0, extent, axis=direction)

    return jnp.maximum(speed, 0.0) * differ(lower_faces) + jnp.minimum(speed, 0.0) * differ(upper_faces)


def transport(chemical_log_concentrations, advection_wind):
    def one_species(field):
        summed = jnp.zeros_like(field)
        for direction in range(3):
            widths = [(0, 0), (0, 0), (0, 0)]
            widths[direction] = (3, 3)
            padded = jnp.pad(field, widths, mode="wrap")
            summed = summed + upwind(padded, direction, field.shape[direction], advection_wind[direction])
        return field - flow_step * summed

    return lax.map(one_species, chemical_log_concentrations)


def fence_period(values):
    return lax.optimization_barrier(values.astype(jnp.bfloat16)).astype(jnp.float32)


def integrate(start_rows, theta_rows, forward_wide, net_wide, arrhenius_log_coefficient, arrhenius_energy):
    highest = lax.Precision.HIGHEST
    bias = arrhenius_log_coefficient[None, :, None] - arrhenius_energy[None, :, None] * theta_rows[:, None, :]
    current = start_rows
    for sub_index in range(SUBSTEPS):
        features = fence_period(current)
        exponent = jnp.einsum("rs,psn->prn", forward_wide, features, precision=highest) + bias
        rates = fence_period(jnp.exp(exponent))
        source = fence_period(jnp.einsum("sr,prn->psn", net_wide, rates, precision=highest))
        current = current + sub_step * source
    return fence_period(current - start_rows)


def reference(chemical_log_concentrations, advection_wind, inverse_thermal_scale, kinetics_column_switch, kinetic_exponents, arrhenius_log_coefficient, arrhenius_energy, stoichiometric_production, formation_heat, streamwise_tucker_basis):
    transported = transport(chemical_log_concentrations, advection_wind)
    forward_wide = kinetic_exponents.astype(jnp.float32)
    net_wide = stoichiometric_production.astype(jnp.float32)
    highest = lax.Precision.HIGHEST
    rotation_voxels = fence_period(inverse_thermal_scale).reshape(GRID_WIDTH_EAST, GRID_WIDTH_NORTH, COLUMN_TALLY, COLUMN_DEPTH)
    state = transported.reshape(SPECIES, GRID_WIDTH_EAST, GRID_WIDTH_NORTH, COLUMN_TALLY, COLUMN_DEPTH)
    total_hot = LOAD * N_GY * N_GZ * N_GX
    block_rows = math.gcd(total_hot, 512)
    for section in range(CHEMISTRY_CALLS):
        first_index, second_index, third_index = jnp.nonzero(kinetics_column_switch[section], size=total_hot)
        first_index = first_index.astype(jnp.int32)
        second_index = second_index.astype(jnp.int32)
        third_index = third_index.astype(jnp.int32)
        rows = state[:, first_index, second_index, third_index, :].transpose(1, 0, 2)
        start_rows = fence_period(rows)
        theta_rows = rotation_voxels[first_index, second_index, third_index, :]
        start_blocks = start_rows.reshape(total_hot // block_rows, block_rows, SPECIES, COLUMN_DEPTH)
        theta_blocks = theta_rows.reshape(total_hot // block_rows, block_rows, COLUMN_DEPTH)

        def one_block(pair):
            return integrate(pair[0], pair[1], forward_wide, net_wide, arrhenius_log_coefficient, arrhenius_energy)

        increment = lax.map(one_block, (start_blocks, theta_blocks)).reshape(total_hot, SPECIES, COLUMN_DEPTH)
        state = state.at[:, first_index, second_index, third_index, :].add(increment.transpose(1, 0, 2))
    species_out = state.reshape(SPECIES, GRID_WIDTH_EAST, GRID_WIDTH_NORTH, GRID_WIDTH_UPWARD)
    heat_release = -jnp.sum(formation_heat[:, None, None, None] * (species_out - transported), axis=0)
    projected = jnp.einsum("xm,xyz->myz", streamwise_tucker_basis, heat_release, precision=highest)
    core = projected.reshape(MODES, GRID_WIDTH_NORTH // CY, CY, GRID_WIDTH_UPWARD).transpose(1, 0, 2, 3)
    return species_out, core
```

```python
import jax
import jax.numpy as jnp
from jax import lax
from jax.experimental import pallas as pl
from jax.experimental.pallas import tpu as pltpu
from jax.sharding import PartitionSpec as P

SUBSTEPS = 2
OCTET = 8
LANES = 128

flow_step = 0.15
sub_step = 0.04
smooth_eps = 1e-06


def shift(array, axis, by):
    count = lax.axis_size(axis)
    return lax.ppermute(array, axis, [(i, (i + by) % count) for i in range(count)])


def indicators(before, after):
    curve = after - before
    bent = 1.5 * curve
    centre = (curve * curve + 0.75 * smooth_eps) + 0.75 * (before * after)
    return centre + after * bent, centre, centre - before * bent


def faces(left, middle, right, third_low, third_high):
    ml = middle * left
    mr = middle * right
    lr = left * right
    ml = ml * ml
    mr = mr * mr
    lr = lr * lr
    total = (ml + mr) + 6.0 * lr
    first = ml * third_high
    second = mr * third_low
    both = 2.0 * (first + second)
    return (both + first) / (total + 2.0 * ml), (both + second) / (total + 2.0 * mr)


def line(load, count, speed, put):
    def kept(function):
        known = {}

        def get(i):
            if i not in known:
                known[i] = function(i)
            return known[i]

        return get

    u = kept(load)
    d = kept(lambda i: u(i + 1) - u(i))
    second = kept(lambda i: d(i) - d(i - 1))
    third = kept(lambda i: second(i) - second(i - 1))
    ind = kept(lambda i: indicators(d(i - 1), d(i)))
    both = kept(
        lambda i: faces(ind(i - 1)[0], ind(i)[1], ind(i + 1)[2], third(i), third(i + 1))
    )
    for i in range(count):
        v = speed(i)
        bend = jnp.where(
            v > 0.0,
            third(i) + (both(i)[0] - both(i - 1)[0]),
            third(i + 1) - (both(i + 1)[1] - both(i)[1]),
        )
        put(i, v * (3.0 * (d(i) + d(i - 1)) - bend))


def groups_of(species):
    return list(range(0, species - OCTET, OCTET)) + [species - OCTET]


def rounded(array):
    return array.astype(jnp.bfloat16).astype(jnp.float32)


def split_three(array):
    first = rounded(array)
    second = rounded(array - first)
    return [first, second, rounded(array - first - second)]


def prep_kernel(
    u_ref, orders_ref, log_ref, energy_ref, net_in_ref, heat_in_ref, *refs,
    species, width_x, width_y, row_tiles, spans,
):
    chunk_refs = refs[: len(spans)]
    low_ref, high_ref, zpack_ref, order_ref, net_ref, heat_ref, zwide_ref = refs[len(spans) :]
    pencils = width_x * width_y
    for c, (y0, y1) in enumerate(spans):
        for x in range(width_x):
            chunk_refs[c][:, x] = u_ref[
                :, x * width_y + y0 : x * width_y + y1, :
            ].astype(jnp.bfloat16)
    flat = u_ref.reshape(species * pencils, LANES)
    for g, s0 in enumerate(groups_of(species)):
        for x in range(width_x):
            for k in range(3):
                low_ref[x * 3 + k, g * OCTET : (g + 1) * OCTET, :] = flat[
                    pl.ds(s0 * pencils + x * width_y + k, OCTET, stride=pencils), :
                ].astype(jnp.bfloat16)
                high_ref[x * 3 + k, g * OCTET : (g + 1) * OCTET, :] = flat[
                    pl.ds(s0 * pencils + x * width_y + width_y - 3 + k, OCTET, stride=pencils), :
                ].astype(jnp.bfloat16)
    k = lax.broadcasted_iota(jnp.int32, (OCTET, LANES), 0)
    z = lax.broadcasted_iota(jnp.int32, (OCTET, LANES), 1)
    pick = jnp.where(
        ((k < 3) & (z == k)) | ((k >= 3) & (k < 6) & (z == LANES - 6 + k)), 1.0, 0.0
    ).astype(jnp.bfloat16)
    rows = species * pencils
    slots = zpack_ref.shape[0] // 6
    zwide_ref[...] = jnp.zeros(zwide_ref.shape, jnp.float32)
    for j in range(row_tiles):
        j0 = min(j * LANES, rows - LANES)
        block = flat[j0 : j0 + LANES, :].astype(jnp.bfloat16)
        ends = lax.dot_general(
            pick, block, (((1,), (1,)), ((), ())), preferred_element_type=jnp.float32
        )
        zwide_ref[pl.ds(j, OCTET, stride=slots), :] = ends
    zpack_ref[...] = zwide_ref[: 6 * slots, :].astype(jnp.bfloat16)

    reactions, wide = order_ref.shape
    row = lax.broadcasted_iota(jnp.int32, (species, wide), 0)
    col = lax.broadcasted_iota(jnp.int32, (species, wide), 1)
    same = jnp.where(row == col, 1.0, 0.0).astype(jnp.bfloat16)
    bias = split_three(-energy_ref[...]) + split_three(log_ref[...])
    bias = jnp.concatenate(bias + [jnp.zeros((2, reactions), jnp.float32)], axis=0)
    row = lax.broadcasted_iota(jnp.int32, (OCTET, wide), 0)
    col = lax.broadcasted_iota(jnp.int32, (OCTET, wide), 1)
    late = jnp.where(col == wide - OCTET + row, 1.0, 0.0).astype(jnp.bfloat16)
    order_ref[...] = (
        jnp.dot(orders_ref[...], same, preferred_element_type=jnp.float32)
        + lax.dot_general(
            bias.astype(jnp.bfloat16), late, (((0,), (0,)), ((), ())),
            preferred_element_type=jnp.float32,
        )
    ).astype(jnp.bfloat16)
    row = lax.broadcasted_iota(jnp.int32, (wide, species), 0)
    col = lax.broadcasted_iota(jnp.int32, (wide, species), 1)
    same = jnp.where(row == col, 1.0, 0.0).astype(jnp.bfloat16)
    net_ref[...] = jnp.dot(
        same, net_in_ref[...], preferred_element_type=jnp.float32
    ).astype(jnp.bfloat16)
    heats = split_three(-heat_in_ref[...])
    heats = jnp.concatenate(heats + [jnp.zeros((5, species), jnp.float32)], axis=0)
    heat_ref[...] = lax.dot_general(
        heats.astype(jnp.bfloat16), same, (((1,), (1,)), ((), ())),
        preferred_element_type=jnp.float32,
    ).astype(jnp.bfloat16)


def flow_kernel(
    u_ref, low_ref, high_ref, zlow_ref, zhigh_ref, v_ref,
    out_ref, acc_ref, across_ref, speed_ref, moved_ref,
    *, species, width_x, width_y, row_tiles, slots, pitch,
):
    pencils = width_x * width_y
    rows = species * pencils
    flat = u_ref.reshape(rows, LANES)
    count = len(groups_of(species))

    def first_row(j):
        return min(j * LANES, rows - LANES)

    for j in range(row_tiles):
        j0 = first_row(j)
        across_ref[j * pitch : j * pitch + LANES, :] = flat[j0 : j0 + LANES, :].T
    for j in range(row_tiles, slots):
        across_ref[j * pitch : (j + 1) * pitch, :] = jnp.zeros((pitch, LANES), jnp.float32)
        speed_ref[j * pitch : (j + 1) * pitch, :] = jnp.zeros((pitch, LANES), jnp.float32)
    wind = v_ref[2]
    turned = {}
    for j in range(row_tiles):
        p0 = first_row(j) % pencils
        if p0 not in turned:
            pieces, need, at = [], LANES, p0
            while need > 0:
                take = min(need, pencils - at)
                pieces.append(wind[at : at + take])
                need, at = need - take, 0
            turned[p0] = jnp.concatenate(pieces, axis=0).T
    for j in range(row_tiles):
        speed_ref[j * pitch : j * pitch + LANES, :] = turned[first_row(j) % pencils]

    def north(step, carry):
        g = step // width_x
        x = step % width_x
        s0 = jnp.minimum(g * OCTET, species - OCTET)
        base = s0 * pencils + x * width_y
        g0 = pl.multiple_of(g * OCTET, OCTET)

        def load(i):
            if i < 0:
                return low_ref[x * 3 + i + 3, pl.ds(g0, OCTET), :].astype(jnp.float32)
            if i >= width_y:
                return high_ref[x * 3 + i - width_y, pl.ds(g0, OCTET), :].astype(jnp.float32)
            return flat[pl.ds(base + i, OCTET, stride=pencils), :]

        def speed(i):
            return jnp.broadcast_to(v_ref[1, pl.ds(x * width_y + i, 1), :], (OCTET, LANES))

        def put(i, value):
            acc_ref[pl.ds(base + i, OCTET, stride=pencils), :] = value

        line(load, width_y, speed, put)
        return carry

    lax.fori_loop(0, count * width_x, north, 0)

    def upward(q, carry):
        t0 = pl.multiple_of(q * OCTET, OCTET)
        base = t0 * pitch

        def load(i):
            if i < 0:
                return zlow_ref[pl.ds((i + 6) * slots + t0, OCTET), :].astype(jnp.float32)
            if i >= LANES:
                return zhigh_ref[pl.ds((i - LANES) * slots + t0, OCTET), :].astype(jnp.float32)
            return across_ref[pl.ds(base + i, OCTET, stride=pitch), :]

        def speed(i):
            return speed_ref[pl.ds(base + i, OCTET, stride=pitch), :]

        def put(i, value):
            moved_ref[pl.ds(base + i, OCTET, stride=pitch), :] = value

        line(load, LANES, speed, put)
        return carry

    lax.fori_loop(0, slots // OCTET, upward, 0)

    out_flat = out_ref.reshape(rows, LANES)
    for j in range(row_tiles):
        j0 = first_row(j)
        at = slice(j0, j0 + LANES)
        moved = moved_ref[j * pitch : j * pitch + LANES, :].T + acc_ref[at, :]
        out_flat[at, :] = flat[at, :] - (flow_step / 6.0) * moved


def chunk_kernel(
    me_ref, hot_ref, u_ref, part_ref, low_ref, high_ref, v_ref, theta_ref,
    order_ref, net_ref, heat_ref, basis_ref, *refs,
    species, width_x, span, members, share, first, last,
):
    refs = list(refs)
    before_ref = None if first else refs.pop(0)
    out_ref = refs.pop(0)
    cells_ref = refs.pop()
    release_ref = refs.pop() if last else refs.pop(0)
    y0, y1 = span
    width = y1 - y0
    octets = width // OCTET
    together = 2 if octets == 1 else 1

    def east(step, carry):
        for extra in range(together):
            s = jnp.minimum(step * together, species - together) + extra
            for o in range(octets):
                at = slice(o * OCTET, (o + 1) * OCTET)

                def load(i):
                    if i < 0:
                        return low_ref[s, i + width_x, at].astype(jnp.float32)
                    if i >= width_x:
                        return high_ref[s, i - width_x, at].astype(jnp.float32)
                    return u_ref[s, i, at]

                def put(i, value):
                    out_ref[s, i, at] = part_ref[s, i, at] - (flow_step / 6.0) * value

                line(load, width_x, lambda i: v_ref[i, at], put)
        return carry

    lax.fori_loop(0, -(-species // together), east, 0)

    if first:
        release_ref[...] = jnp.zeros(release_ref.shape, jnp.float32)
    else:
        release_ref[...] = before_ref[...]
    rows = width_x * width
    flat = out_ref.reshape(species * rows, LANES)
    starts = [(s0, min(OCTET, species - s0)) for s0 in range(0, species, OCTET)]
    sublane = lax.broadcasted_iota(jnp.int32, (OCTET, LANES), 0)
    order = order_ref[...]
    net = net_ref[...]
    heat = heat_ref[...]
    depth = order.shape[1]
    for block in range(width_x * octets):
        x, o = block // octets, block % octets
        for y in range(OCTET):
            cols = slice(y * LANES, (y + 1) * LANES)
            at = x * width + o * OCTET + y
            cells_ref[block, depth - 2 * OCTET : depth - OCTET, cols] = jnp.zeros(
                (OCTET, LANES), jnp.float32
            )
            for s0, size in starts:
                cells_ref[block, s0 : s0 + size, cols] = flat[
                    pl.ds(s0 * rows + at, size, stride=rows), :
                ]
            theta = jnp.broadcast_to(
                theta_ref[x, o * OCTET + y : o * OCTET + y + 1, :], (OCTET, LANES)
            )
            cells_ref[block, depth - OCTET :, cols] = jnp.where(
                sublane < 3, theta, jnp.where(sublane < 6, 1.0, 0.0)
            )
    for block in range(width_x * octets):
        x, o = block // octets, block % octets
        start = rounded(cells_ref[block])
        current = start
        for _ in range(SUBSTEPS):
            features = current.astype(jnp.bfloat16)
            exponent = jnp.dot(order, features, preferred_element_type=jnp.float32)
            rates = jnp.exp(exponent).astype(jnp.bfloat16)
            source = jnp.dot(net, rates, preferred_element_type=jnp.float32)
            current = current + sub_step * rounded(source)
        increment = rounded(current - start)
        for y in range(OCTET):
            cols = slice(y * LANES, (y + 1) * LANES)
            row = y0 + o * OCTET + y
            at = x * width + o * OCTET + y
            gain = jnp.where(hot_ref[x, 0, row] > 0, increment[:, cols], 0.0)
            for s0, size in starts:
                flat[pl.ds(s0 * rows + at, size, stride=rows), :] = (
                    cells_ref[block, s0 : s0 + size, cols] + gain[s0 : s0 + size, :]
                )
            sums = jnp.dot(heat, gain.astype(jnp.bfloat16), preferred_element_type=jnp.float32)
            release_ref[row // share, x, row % share : row % share + 1, :] = (
                sums[0:1] + sums[1:2] + sums[2:3]
            )
    if last:
        modes = basis_ref.shape[1]
        for k in range(members):
            for x in range(width_x):
                release_ref[k, x, OCTET - 1 :, 0:modes] = basis_ref[x : x + 1, :]
        for j in range(members):
            refs[j][...] = release_ref[lax.rem(me_ref[0] + j, members)]


def core_kernel(*refs, members, width_x, share, modes):
    parts = refs[:members]
    out_ref, rows_ref = refs[members:]
    lines = members * width_x
    padded = rows_ref.shape[0] // OCTET
    for j in range(members):
        for x in range(width_x):
            at = (j * width_x + x) * OCTET
            rows_ref[at : at + OCTET, :] = parts[j][x]
    if padded > lines:
        rows_ref[lines * OCTET :, :] = jnp.zeros(((padded - lines) * OCTET, LANES), jnp.float32)

    def gather(y):
        return jnp.concatenate(
            [
                rows_ref[pl.ds(a * OCTET * OCTET + y, OCTET, stride=OCTET), :]
                for a in range(padded // OCTET)
            ],
            axis=0,
        )

    basis = gather(OCTET - 1).T[:modes]
    for y in range(share):
        out_ref[y] = jnp.dot(
            basis, gather(y), preferred_element_type=jnp.float32, precision=lax.Precision.HIGHEST
        )


def body(
    chemical_log_concentrations,
    advection_wind,
    inverse_thermal_scale,
    kinetics_column_switch,
    kinetic_exponents,
    arrhenius_log_coefficient,
    arrhenius_energy,
    stoichiometric_production,
    formation_heat,
    streamwise_tucker_basis,
):
    species, width_x, width_y, depth = chemical_log_concentrations.shape
    pencils = width_x * width_y
    rows = species * pencils
    row_tiles = -(-rows // LANES)
    slots = -(-row_tiles // OCTET) * OCTET
    pitch = LANES + OCTET
    padded = len(groups_of(species)) * OCTET
    reactions = kinetic_exponents.shape[0]
    members = lax.axis_size("gx")
    share = width_y // members
    modes = streamwise_tucker_basis.shape[1]
    cut = width_y - OCTET
    spans = [(0, cut), (cut, width_y)]
    vmem = pl.BlockSpec(memory_space=pltpu.VMEM)
    smem = pl.BlockSpec(memory_space=pltpu.SMEM)
    flat_u = chemical_log_concentrations.reshape(species, pencils, depth)
    wind = advection_wind.reshape(3, pencils, depth)

    def chunk(span):
        return jax.ShapeDtypeStruct((species, width_x, span[1] - span[0], LANES), jnp.bfloat16)

    side = jax.ShapeDtypeStruct((width_x * 3, padded, LANES), jnp.bfloat16)
    *chunks, y_low, y_high, z_own, order, net, heat = pl.pallas_call(
        lambda *refs: prep_kernel(
            *refs, species=species, width_x=width_x, width_y=width_y, row_tiles=row_tiles,
            spans=spans,
        ),
        in_specs=[vmem] * 6,
        out_specs=[vmem] * (len(spans) + 6),
        out_shape=[chunk(span) for span in spans]
        + [
            side,
            side,
            jax.ShapeDtypeStruct((6 * slots, LANES), jnp.bfloat16),
            jax.ShapeDtypeStruct((reactions, padded + OCTET), jnp.bfloat16),
            jax.ShapeDtypeStruct((padded + OCTET, reactions), jnp.bfloat16),
            jax.ShapeDtypeStruct((OCTET, padded + OCTET), jnp.bfloat16),
        ],
        scratch_shapes=[pltpu.VMEM((OCTET * slots, LANES), jnp.float32)],
        name="prep",
    )(
        flat_u,
        kinetic_exponents,
        arrhenius_log_coefficient.reshape(1, reactions),
        arrhenius_energy.reshape(1, reactions),
        stoichiometric_production,
        formation_heat.reshape(1, species),
    )

    x_low = [shift(part, "gx", 1) for part in chunks]
    x_high = [shift(part, "gx", -1) for part in chunks]
    low_rows = shift(y_high, "gy", 1)
    high_rows = shift(y_low, "gy", -1)
    z_low = shift(z_own, "gz", 1)
    z_high = z_low if lax.axis_size("gz") == 2 else shift(z_own, "gz", -1)

    cells = rows * depth
    part = pl.pallas_call(
        lambda *refs: flow_kernel(
            *refs, species=species, width_x=width_x, width_y=width_y, row_tiles=row_tiles,
            slots=slots, pitch=pitch,
        ),
        in_specs=[vmem] * 6,
        out_specs=vmem,
        out_shape=jax.ShapeDtypeStruct((species, pencils, depth), jnp.float32),
        scratch_shapes=[
            pltpu.VMEM((rows, LANES), jnp.float32),
            pltpu.VMEM((slots * pitch, LANES), jnp.float32),
            pltpu.VMEM((slots * pitch, LANES), jnp.float32),
            pltpu.VMEM((slots * pitch, LANES), jnp.float32),
        ],
        cost_estimate=pl.CostEstimate(
            flops=cells * 130, bytes_accessed=cells * 8, transcendentals=cells * 4
        ),
        name="flow",
    )(flat_u, low_rows, high_rows, z_low, z_high, wind)
    state = part.reshape(species, width_x, width_y, depth)

    hot = jnp.swapaxes(kinetics_column_switch, 2, 3).reshape(width_x, 1, width_y)
    me = lax.axis_index("gx").astype(jnp.int32).reshape(1)
    release = None
    tile = jax.ShapeDtypeStruct((width_x, OCTET, LANES), jnp.float32)
    pile = jax.ShapeDtypeStruct((members, width_x, OCTET, LANES), jnp.float32)
    for c, span in enumerate(spans):
        width = span[1] - span[0]
        at = span[0] // width
        first, last = c == 0, c == len(spans) - 1
        block = pl.BlockSpec((species, width_x, width, LANES), lambda i, a=at: (0, 0, a, 0))
        near = pl.BlockSpec((width_x, width, LANES), lambda i, a=at: (0, a, 0))
        wind_block = pl.BlockSpec(
            (None, width_x, width, LANES), lambda i, a=at: (0, 0, a, 0)
        )

        def whole(shape):
            return pl.BlockSpec(shape, lambda i, n=len(shape): (0,) * n)

        outs = [tile] * members if last else [pile]
        fixed = [x_low[c], x_high[c]], [order, net, heat, streamwise_tucker_basis]
        results = pl.pallas_call(
            lambda *refs, first=first, last=last, span=span: chunk_kernel(
                *refs, species=species, width_x=width_x, span=span, members=members,
                share=share, first=first, last=last,
            ),
            grid=(1,),
            in_specs=[smem, smem, block, block]
            + [whole(a.shape) for a in fixed[0]]
            + [wind_block, near]
            + [whole(a.shape) for a in fixed[1]]
            + ([] if first else [whole(pile.shape)]),
            out_specs=[block] + [whole(a.shape) for a in outs],
            out_shape=[jax.ShapeDtypeStruct(state.shape, jnp.float32)] + outs,
            scratch_shapes=([pltpu.VMEM(pile.shape, jnp.float32)] if last else [])
            + [
                pltpu.VMEM(
                    (width_x * width // OCTET, padded + OCTET, OCTET * LANES), jnp.float32
                )
            ],
            input_output_aliases={3: 0},
            cost_estimate=pl.CostEstimate(
                flops=cells * 60, bytes_accessed=cells * 4, transcendentals=cells * 4
            ),
            name=f"chunk{c}",
        )(
            me, hot, chemical_log_concentrations, state, *fixed[0], advection_wind,
            inverse_thermal_scale, *fixed[1], *([] if first else [release]),
        )
        state = results[0]
        release = results[1]
    pieces = results[1:]

    moved = [pieces[0]] + [shift(pieces[j], "gx", j) for j in range(1, members)]
    lines = -(-members * width_x // OCTET) * OCTET
    core = pl.pallas_call(
        lambda *refs: core_kernel(
            *refs, members=members, width_x=width_x, share=share, modes=modes
        ),
        in_specs=[vmem] * members,
        out_specs=vmem,
        out_shape=jax.ShapeDtypeStruct((share, modes, depth), jnp.float32),
        scratch_shapes=[pltpu.VMEM((lines * OCTET, LANES), jnp.float32)],
        name="core",
    )(*moved)
    return (state, core.transpose(1, 0, 2)[None])


def solution(mesh):
    placed = (
        P(None, "gx", "gy", "gz"),
        P(None, "gx", "gy", "gz"),
        P("gx", "gy", "gz"),
        P(None, "gx", "gy", "gz"),
        P(),
        P(),
        P(),
        P(),
        P(),
        P("gx", None),
    )
    return jax.shard_map(
        body,
        mesh=mesh,
        in_specs=placed,
        out_specs=(P(None, "gx", "gy", "gz"), P("gy", None, "gx", "gz")),
        check_vma=False,
    )
```

```python
import jax
import jax.numpy as jnp
from jax import lax
from jax.experimental import pallas as pl
from jax.experimental.pallas import tpu as pltpu
from jax.sharding import PartitionSpec as P

SUBSTEPS = 2
OCTET = 8
LANES = 128

flow_step = 0.15
sub_step = 0.04
smooth_eps = 1e-06


def shift(array, axis, by):
    count = lax.axis_size(axis)
    return lax.ppermute(array, axis, [(i, (i + by) % count) for i in range(count)])


def swap(array, axis, late):
    count = lax.axis_size(axis)
    pairs = [(i, (i + 1) % count) for i in range(late, count + late, 2)]
    pairs = [(a % count, b % count) for a, b in pairs]
    return lax.ppermute(array, axis, pairs + [(b, a) for a, b in pairs])


def close(array):
    return pltpu.with_memory_space_constraint(array, pltpu.VMEM)


def far(array):
    return pltpu.with_memory_space_constraint(array, pltpu.HBM)


def indicators(before, after):
    curve = after - before
    bent = 1.5 * curve
    centre = (curve * curve + 0.75 * smooth_eps) + 0.75 * (before * after)
    return centre + after * bent, centre, centre - before * bent


def faces(left, middle, right, third_low, third_high):
    ml = middle * left
    mr = middle * right
    lr = left * right
    ml = ml * ml
    mr = mr * mr
    lr = lr * lr
    total = (ml + mr) + 6.0 * lr
    first = ml * third_high
    second = mr * third_low
    both = 2.0 * (first + second)
    return (both + first) / (total + 2.0 * ml), (both + second) / (total + 2.0 * mr)


def line(load, count, speed, put):
    def kept(function):
        known = {}

        def get(i):
            if i not in known:
                known[i] = function(i)
            return known[i]

        return get

    u = kept(load)
    d = kept(lambda i: u(i + 1) - u(i))
    second = kept(lambda i: d(i) - d(i - 1))
    third = kept(lambda i: second(i) - second(i - 1))
    ind = kept(lambda i: indicators(d(i - 1), d(i)))
    both = kept(
        lambda i: faces(ind(i - 1)[0], ind(i)[1], ind(i + 1)[2], third(i), third(i + 1))
    )
    for i in range(count):
        v = speed(i)
        bend = jnp.where(
            v > 0.0,
            third(i) + (both(i)[0] - both(i - 1)[0]),
            third(i + 1) - (both(i + 1)[1] - both(i)[1]),
        )
        put(i, v * (3.0 * (d(i) + d(i - 1)) - bend))


def groups_of(species):
    return list(range(0, species - OCTET, OCTET)) + [species - OCTET]


def rounded(array):
    return array.astype(jnp.bfloat16).astype(jnp.float32)


def split_three(array):
    first = rounded(array)
    second = rounded(array - first)
    return [first, second, rounded(array - first - second)]


def prep_kernel(
    spot_ref, u_ref, *refs,
    species, width_x, width_y, row_tiles, spans,
):
    sources, refs = refs[:7], refs[7:]
    chunk_refs, refs = refs[: len(spans)], refs[len(spans) :]
    early_ref, late_ref, zpack_ref, order_ref, net_ref, heat_ref, wind_ref, scale_ref = refs[:8]
    zwide_ref, orders_ref, log_ref, energy_ref, net_in_ref, heat_in_ref, sems = refs[8:]
    targets = (wind_ref, scale_ref, orders_ref, log_ref, energy_ref, net_in_ref, heat_in_ref)
    copies = [
        pltpu.make_async_copy(source, target, sems.at[i])
        for i, (source, target) in enumerate(zip(sources, targets))
    ]
    for copy in copies:
        copy.start()
    pencils = width_x * width_y
    for c, (y0, y1) in enumerate(spans):
        for x in range(width_x):
            chunk_refs[c][:, x] = u_ref[
                :, x * width_y + y0 : x * width_y + y1, :
            ].astype(jnp.bfloat16)
    flat = u_ref.reshape(species * pencils, LANES)
    odd = lax.rem(spot_ref[0], 2)
    for g, s0 in enumerate(groups_of(species)):
        for x in range(width_x):
            for k in range(3):
                at = s0 * pencils + x * width_y + k
                shown = (x * 3 + k, slice(g * OCTET, (g + 1) * OCTET))
                early_ref[shown] = flat[
                    pl.ds(at + (1 - odd) * (width_y - 3), OCTET, stride=pencils), :
                ].astype(jnp.bfloat16)
                late_ref[shown] = flat[
                    pl.ds(at + odd * (width_y - 3), OCTET, stride=pencils), :
                ].astype(jnp.bfloat16)
    k = lax.broadcasted_iota(jnp.int32, (OCTET, LANES), 0)
    z = lax.broadcasted_iota(jnp.int32, (OCTET, LANES), 1)
    pick = jnp.where(
        ((k < 3) & (z == k)) | ((k >= 3) & (k < 6) & (z == LANES - 6 + k)), 1.0, 0.0
    ).astype(jnp.bfloat16)
    rows = species * pencils
    slots = zpack_ref.shape[0] // 6
    zwide_ref[...] = jnp.zeros(zwide_ref.shape, jnp.float32)
    for j in range(row_tiles):
        j0 = min(j * LANES, rows - LANES)
        block = flat[j0 : j0 + LANES, :].astype(jnp.bfloat16)
        ends = lax.dot_general(
            pick, block, (((1,), (1,)), ((), ())), preferred_element_type=jnp.float32
        )
        zwide_ref[pl.ds(j, OCTET, stride=slots), :] = ends
    zpack_ref[...] = zwide_ref[: 6 * slots, :].astype(jnp.bfloat16)

    for copy in copies:
        copy.wait()
    reactions, wide = order_ref.shape
    row = lax.broadcasted_iota(jnp.int32, (species, wide), 0)
    col = lax.broadcasted_iota(jnp.int32, (species, wide), 1)
    same = jnp.where(row == col, 1.0, 0.0).astype(jnp.bfloat16)
    bias = split_three(-energy_ref[...]) + split_three(log_ref[...])
    bias = jnp.concatenate(bias + [jnp.zeros((2, reactions), jnp.float32)], axis=0)
    row = lax.broadcasted_iota(jnp.int32, (OCTET, wide), 0)
    col = lax.broadcasted_iota(jnp.int32, (OCTET, wide), 1)
    late = jnp.where(col == wide - OCTET + row, 1.0, 0.0).astype(jnp.bfloat16)
    order_ref[...] = (
        lax.dot_general(
            orders_ref[...], same, (((0,), (0,)), ((), ())), preferred_element_type=jnp.float32
        )
        + lax.dot_general(
            bias.astype(jnp.bfloat16), late, (((0,), (0,)), ((), ())),
            preferred_element_type=jnp.float32,
        )
    ).astype(jnp.bfloat16)
    row = lax.broadcasted_iota(jnp.int32, (wide, species), 0)
    col = lax.broadcasted_iota(jnp.int32, (wide, species), 1)
    same = jnp.where(row == col, 1.0, 0.0).astype(jnp.bfloat16)
    net_ref[...] = jnp.dot(
        same, net_in_ref[...], preferred_element_type=jnp.float32
    ).astype(jnp.bfloat16)
    heats = split_three(-heat_in_ref[...])
    heats = jnp.concatenate(heats + [jnp.zeros((5, species), jnp.float32)], axis=0)
    heat_ref[...] = lax.dot_general(
        heats.astype(jnp.bfloat16), same, (((1,), (1,)), ((), ())),
        preferred_element_type=jnp.float32,
    ).astype(jnp.bfloat16)


def upward_kernel(
    u_ref, zlow_ref, zhigh_ref, v_ref, out_ref, across_ref, speed_ref, moved_ref,
    *, species, pencils, row_tiles, slots, pitch,
):
    rows = species * pencils
    flat = u_ref.reshape(rows, LANES)

    def first_row(j):
        return min(j * LANES, rows - LANES)

    for j in range(row_tiles, slots):
        across_ref[j * pitch : (j + 1) * pitch, :] = jnp.zeros((pitch, LANES), jnp.float32)
        speed_ref[j * pitch : (j + 1) * pitch, :] = jnp.zeros((pitch, LANES), jnp.float32)
    wind = v_ref[2]
    turned = {}
    for j in range(row_tiles):
        p0 = first_row(j) % pencils
        if p0 not in turned:
            strips, need, at = [], LANES, p0
            while need > 0:
                take = min(need, pencils - at)
                strips.append(wind[at : at + take])
                need, at = need - take, 0
            turned[p0] = jnp.concatenate(strips, axis=0).T
    for j in range(row_tiles):
        speed_ref[j * pitch : j * pitch + LANES, :] = turned[first_row(j) % pencils]
    for j in range(row_tiles):
        j0 = first_row(j)
        across_ref[j * pitch : j * pitch + LANES, :] = flat[j0 : j0 + LANES, :].T

    def upward(q, carry):
        t0 = pl.multiple_of(q * OCTET, OCTET)
        base = t0 * pitch

        def load(i):
            if i < 0:
                return zlow_ref[pl.ds((i + 6) * slots + t0, OCTET), :].astype(jnp.float32)
            if i >= LANES:
                return zhigh_ref[pl.ds((i - LANES) * slots + t0, OCTET), :].astype(jnp.float32)
            return across_ref[pl.ds(base + i, OCTET, stride=pitch), :]

        def speed(i):
            return speed_ref[pl.ds(base + i, OCTET, stride=pitch), :]

        def put(i, value):
            moved_ref[pl.ds(base + i, OCTET, stride=pitch), :] = value

        line(load, LANES, speed, put)
        return carry

    lax.fori_loop(0, slots // OCTET, upward, 0)

    for j in range(row_tiles):
        j0 = j * LANES
        size = min(LANES, rows - j0)
        skip = j0 - first_row(j)
        out_ref[j0 : j0 + size, :] = moved_ref[j * pitch : j * pitch + LANES, :].T[skip:]


def north_kernel(
    spot_ref, u_ref, z_ref, early_ref, late_ref, v_ref, out_ref, acc_ref,
    *, species, width_x, width_y,
):
    pencils = width_x * width_y
    rows = species * pencils
    flat = u_ref.reshape(rows, LANES)
    count = len(groups_of(species))
    odd = lax.rem(spot_ref[0], 2) == 1

    def north(step, carry):
        g = step // width_x
        x = step % width_x
        s0 = jnp.minimum(g * OCTET, species - OCTET)
        base = s0 * pencils + x * width_y
        g0 = pl.multiple_of(g * OCTET, OCTET)

        def load(i):
            if i < 0 or i >= width_y:
                at = (x * 3 + (i + 3 if i < 0 else i - width_y), pl.ds(g0, OCTET))
                ours, other = early_ref[at], late_ref[at]
                if i >= width_y:
                    ours, other = other, ours
                return jnp.where(odd, ours.astype(jnp.float32), other.astype(jnp.float32))
            return flat[pl.ds(base + i, OCTET, stride=pencils), :]

        def speed(i):
            return jnp.broadcast_to(v_ref[1, pl.ds(x * width_y + i, 1), :], (OCTET, LANES))

        def put(i, value):
            acc_ref[pl.ds(base + i, OCTET, stride=pencils), :] = value

        line(load, width_y, speed, put)
        return carry

    lax.fori_loop(0, count * width_x, north, 0)

    def close_up(s, carry):
        at = pl.ds(pl.multiple_of(s * pencils, OCTET), pencils)
        out_ref[at, :] = flat[at, :] - (flow_step / 6.0) * (acc_ref[at, :] + z_ref[at, :])
        return carry

    lax.fori_loop(0, species, close_up, 0)


def chunk_kernel(
    me_ref, hot_ref, u_ref, part_ref, early_ref, late_ref, wind_ref, scale_ref,
    order_ref, net_ref, heat_ref, basis_ref, *refs,
    species, width_x, span, members, share, first, last,
):
    refs = list(refs)
    before_ref = None
    if not first:
        before_ref = refs.pop(0)
        refs.pop(0)
    out_hbm = refs.pop(0)
    out_ref, cells_ref, out_sems = refs[-3:]
    refs = refs[:-3]
    release_ref = refs.pop() if last else refs.pop(0)
    y0, y1 = span
    width = y1 - y0
    octets = width // OCTET
    together = 2 if octets == 1 else 1
    odd = lax.rem(me_ref[0], 2)
    width_y = scale_ref.shape[1]
    u_ref = u_ref.reshape(species, width_x, width_y, LANES)
    part_ref = part_ref.reshape(species, width_x, width_y, LANES)

    def east(s, low_ref, high_ref):
        for o in range(octets):
            at = slice(o * OCTET, (o + 1) * OCTET)
            there = slice(y0 + o * OCTET, y0 + (o + 1) * OCTET)

            def load(i):
                if i < 0:
                    return low_ref[s, i + width_x, at].astype(jnp.float32)
                if i >= width_x:
                    return high_ref[s, i - width_x, at].astype(jnp.float32)
                return u_ref[s, i, there]

            def put(i, value):
                out_ref[s, i, at] = part_ref[s, i, there] - (flow_step / 6.0) * value

            line(load, width_x, lambda i: wind_ref[0, i * width_y + there.start : i * width_y + there.stop], put)

    for parity, low_ref, high_ref in ((0, late_ref, early_ref), (1, early_ref, late_ref)):

        @pl.when(odd == parity)
        def _(low_ref=low_ref, high_ref=high_ref):
            def several(step, carry):
                for extra in range(together):
                    east(step * together + extra, low_ref, high_ref)
                return carry

            lax.fori_loop(0, species // together, several, 0)
            for rest in range(species // together * together, species):
                east(rest, low_ref, high_ref)

    if first:
        release_ref[...] = jnp.zeros(release_ref.shape, jnp.float32)
    else:
        release_ref[...] = before_ref[...]
    rows = width_x * width
    flat = out_ref.reshape(species * rows, LANES)
    starts = [(s0, min(OCTET, species - s0)) for s0 in range(0, species, OCTET)]
    sublane = lax.broadcasted_iota(jnp.int32, (OCTET, LANES), 0)
    order = order_ref[...]
    net = net_ref[...]
    heat = heat_ref[...]
    depth = order.shape[1]
    for block in range(width_x * octets):
        x, o = block // octets, block % octets
        for y in range(OCTET):
            cols = slice(y * LANES, (y + 1) * LANES)
            at = x * width + o * OCTET + y
            cells_ref[block, depth - 2 * OCTET : depth - OCTET, cols] = jnp.zeros(
                (OCTET, LANES), jnp.float32
            )
            for s0, size in starts:
                cells_ref[block, s0 : s0 + size, cols] = flat[
                    pl.ds(s0 * rows + at, size, stride=rows), :
                ]
            theta = jnp.broadcast_to(
                scale_ref[x, y0 + o * OCTET + y : y0 + o * OCTET + y + 1, :], (OCTET, LANES)
            )
            cells_ref[block, depth - OCTET :, cols] = jnp.where(
                sublane < 3, theta, jnp.where(sublane < 6, 1.0, 0.0)
            )
    stores = []
    for block in range(width_x * octets):
        x, o = block // octets, block % octets
        start = rounded(cells_ref[block])
        current = start
        for _ in range(SUBSTEPS):
            features = current.astype(jnp.bfloat16)
            exponent = jnp.dot(order, features, preferred_element_type=jnp.float32)
            rates = jnp.exp(exponent).astype(jnp.bfloat16)
            source = jnp.dot(net, rates, preferred_element_type=jnp.float32)
            current = current + sub_step * rounded(source)
        increment = rounded(current - start)
        for y in range(OCTET):
            cols = slice(y * LANES, (y + 1) * LANES)
            row = y0 + o * OCTET + y
            at = x * width + o * OCTET + y
            gain = jnp.where(hot_ref[x, 0, row] > 0, increment[:, cols], 0.0)
            for s0, size in starts:
                flat[pl.ds(s0 * rows + at, size, stride=rows), :] = (
                    cells_ref[block, s0 : s0 + size, cols] + gain[s0 : s0 + size, :]
                )
            sums = jnp.dot(heat, gain.astype(jnp.bfloat16), preferred_element_type=jnp.float32)
            release_ref[row // share, x, row % share : row % share + 1, :] = (
                sums[0:1] + sums[1:2] + sums[2:3]
            )
        if o == octets - 1:
            stores.append(
                pltpu.make_async_copy(
                    out_ref.at[:, x], out_hbm.at[:, x, pl.ds(y0, width)], out_sems.at[x]
                )
            )
            stores[-1].start()
    if last:
        modes = basis_ref.shape[1]
        for k in range(members):
            for x in range(width_x):
                release_ref[k, x, OCTET - 1 :, 0:modes] = basis_ref[x : x + 1, :]
        for j in range(members):
            refs[j][...] = release_ref[lax.rem(me_ref[0] + j, members)]
    for store in stores:
        store.wait()


def core_kernel(*refs, members, width_x, share, modes):
    parts = refs[:members]
    out_ref, rows_ref = refs[members:]
    lines = members * width_x
    padded = rows_ref.shape[0] // OCTET
    for j in range(members):
        for x in range(width_x):
            at = (j * width_x + x) * OCTET
            rows_ref[at : at + OCTET, :] = parts[j][x]
    if padded > lines:
        rows_ref[lines * OCTET :, :] = jnp.zeros(((padded - lines) * OCTET, LANES), jnp.float32)

    def gather(y):
        return jnp.concatenate(
            [
                rows_ref[pl.ds(a * OCTET * OCTET + y, OCTET, stride=OCTET), :]
                for a in range(padded // OCTET)
            ],
            axis=0,
        )

    basis = gather(OCTET - 1).T[:modes]
    for y in range(share):
        out_ref[y] = jnp.dot(
            basis, gather(y), preferred_element_type=jnp.float32, precision=lax.Precision.HIGHEST
        )


def body(
    chemical_log_concentrations,
    advection_wind,
    inverse_thermal_scale,
    kinetics_column_switch,
    kinetic_exponents,
    arrhenius_log_coefficient,
    arrhenius_energy,
    stoichiometric_production,
    formation_heat,
    streamwise_tucker_basis,
):
    species, width_x, width_y, depth = chemical_log_concentrations.shape
    pencils = width_x * width_y
    rows = species * pencils
    row_tiles = -(-rows // LANES)
    slots = -(-row_tiles // OCTET) * OCTET
    pitch = LANES + OCTET
    padded = len(groups_of(species)) * OCTET
    reactions = kinetic_exponents.shape[0]
    members = lax.axis_size("gx")
    share = width_y // members
    modes = streamwise_tucker_basis.shape[1]
    cut = width_y - OCTET
    spans = [(0, cut), (cut, width_y)]
    vmem = pl.BlockSpec(memory_space=pltpu.VMEM)
    smem = pl.BlockSpec(memory_space=pltpu.SMEM)
    flat_u = close(chemical_log_concentrations.reshape(species, pencils, depth))
    params = pltpu.CompilerParams(vmem_limit_bytes=32 * 1024 * 1024)

    def chunk(span):
        return jax.ShapeDtypeStruct((species, width_x, span[1] - span[0], LANES), jnp.bfloat16)

    side = jax.ShapeDtypeStruct((width_x * 3, padded, LANES), jnp.bfloat16)
    any_spec = pl.BlockSpec(memory_space=pl.ANY)
    me = lax.axis_index("gx").astype(jnp.int32).reshape(1)
    spot = lax.axis_index("gy").astype(jnp.int32).reshape(1)
    *chunks, y_early, y_late, z_own, order, net, heat, wind, scale = pl.pallas_call(
        lambda *refs: prep_kernel(
            *refs, species=species, width_x=width_x, width_y=width_y, row_tiles=row_tiles,
            spans=spans,
        ),
        in_specs=[smem, vmem] + [any_spec] * 7,
        out_specs=[vmem] * (len(spans) + 8),
        out_shape=[chunk(span) for span in spans]
        + [
            side,
            side,
            jax.ShapeDtypeStruct((6 * slots, LANES), jnp.bfloat16),
            jax.ShapeDtypeStruct((reactions, padded + OCTET), jnp.bfloat16),
            jax.ShapeDtypeStruct((padded + OCTET, reactions), jnp.bfloat16),
            jax.ShapeDtypeStruct((OCTET, padded + OCTET), jnp.bfloat16),
            pltpu.VMEM((3, pencils, depth), jnp.float32),
            pltpu.VMEM((width_x, width_y, depth), jnp.float32),
        ],
        scratch_shapes=[
            pltpu.VMEM((OCTET * slots, LANES), jnp.float32),
            pltpu.VMEM((species, reactions), jnp.bfloat16),
            pltpu.VMEM((1, reactions), jnp.float32),
            pltpu.VMEM((1, reactions), jnp.float32),
            pltpu.VMEM((species, reactions), jnp.bfloat16),
            pltpu.VMEM((1, species), jnp.float32),
            pltpu.SemaphoreType.DMA((7,)),
        ],
        compiler_params=params,
        name="prep",
    )(
        spot,
        flat_u,
        far(advection_wind.reshape(3, pencils, depth)),
        far(inverse_thermal_scale),
        far(kinetic_exponents.T),
        far(arrhenius_log_coefficient.reshape(1, reactions)),
        far(arrhenius_energy.reshape(1, reactions)),
        far(stoichiometric_production),
        far(formation_heat.reshape(1, species)),
    )

    z_low = shift(z_own, "gz", 1)
    z_high = z_low if lax.axis_size("gz") == 2 else shift(z_own, "gz", -1)
    x_late = [swap(chunks[0], "gx", 1)]
    late_rows = swap(y_late, "gy", 1)
    early_rows = swap(y_early, "gy", 0)
    x_early = [swap(part, "gx", 0) for part in chunks]
    x_late += [swap(part, "gx", 1) for part in chunks[1:]]

    cells = rows * depth
    raised = pl.pallas_call(
        lambda *refs: upward_kernel(
            *refs, species=species, pencils=pencils, row_tiles=row_tiles, slots=slots, pitch=pitch
        ),
        in_specs=[vmem] * 4,
        out_specs=vmem,
        out_shape=pltpu.VMEM((rows, depth), jnp.float32),
        scratch_shapes=[pltpu.VMEM((slots * pitch, LANES), jnp.float32)] * 3,
        cost_estimate=pl.CostEstimate(
            flops=cells * 60, bytes_accessed=cells * 8, transcendentals=cells * 2
        ),
        compiler_params=params,
        name="upward",
    )(flat_u, close(z_low), close(z_high), wind)
    part = pl.pallas_call(
        lambda *refs: north_kernel(*refs, species=species, width_x=width_x, width_y=width_y),
        in_specs=[smem] + [vmem] * 5,
        out_specs=vmem,
        out_shape=pltpu.VMEM((rows, depth), jnp.float32),
        scratch_shapes=[pltpu.VMEM((rows, LANES), jnp.float32)],
        cost_estimate=pl.CostEstimate(
            flops=cells * 60, bytes_accessed=cells * 8, transcendentals=cells * 2
        ),
        compiler_params=params,
        name="north",
    )(spot, flat_u, raised, close(early_rows), close(late_rows), wind)
    state = None

    hot = jnp.swapaxes(kinetics_column_switch, 2, 3).reshape(width_x, 1, width_y)
    release = None
    tile = jax.ShapeDtypeStruct((width_x, OCTET, LANES), jnp.float32)
    pile = jax.ShapeDtypeStruct((members, width_x, OCTET, LANES), jnp.float32)
    for c, span in enumerate(spans):
        width = span[1] - span[0]
        first, last = c == 0, c == len(spans) - 1

        outs = [tile] * members if last else [pile]
        results = pl.pallas_call(
            lambda *refs, first=first, last=last, span=span: chunk_kernel(
                *refs, species=species, width_x=width_x, span=span, members=members,
                share=share, first=first, last=last,
            ),
            in_specs=[smem, smem] + [vmem] * 10 + ([] if first else [vmem, any_spec]),
            out_specs=[any_spec] + [vmem] * len(outs),
            out_shape=[jax.ShapeDtypeStruct(chemical_log_concentrations.shape, jnp.float32)] + outs,
            scratch_shapes=([pltpu.VMEM(pile.shape, jnp.float32)] if last else [])
            + [
                pltpu.VMEM((species, width_x, width, LANES), jnp.float32),
                pltpu.VMEM(
                    (width_x * width // OCTET, padded + OCTET, OCTET * LANES), jnp.float32
                ),
                pltpu.SemaphoreType.DMA((width_x,)),
            ],
            input_output_aliases={} if first else {13: 0},
            compiler_params=params,
            cost_estimate=pl.CostEstimate(
                flops=cells * 60, bytes_accessed=cells * 4, transcendentals=cells * 4
            ),
        )(
            me, hot, flat_u, part, close(x_early[c]), close(x_late[c]), wind, scale, order, net, heat, streamwise_tucker_basis,
            *([] if first else [release, state]),
        )
        state = results[0]
        release = results[1]
    pieces = results[1:]

    moved = [pieces[0]] + [close(shift(pieces[j], "gx", j)) for j in range(1, members)]
    lines = -(-members * width_x // OCTET) * OCTET
    core = pl.pallas_call(
        lambda *refs: core_kernel(
            *refs, members=members, width_x=width_x, share=share, modes=modes
        ),
        in_specs=[vmem] * members,
        out_specs=vmem,
        out_shape=jax.ShapeDtypeStruct((share, modes, depth), jnp.float32),
        scratch_shapes=[pltpu.VMEM((lines * OCTET, LANES), jnp.float32)],
        compiler_params=params,
        name="core",
    )(*moved)
    return (state, core.transpose(1, 0, 2)[None])


def solution(mesh):
    placed = (
        P(None, "gx", "gy", "gz"),
        P(None, "gx", "gy", "gz"),
        P("gx", "gy", "gz"),
        P(None, "gx", "gy", "gz"),
        P(),
        P(),
        P(),
        P(),
        P(),
        P("gx", None),
    )
    return jax.shard_map(
        body,
        mesh=mesh,
        in_specs=placed,
        out_specs=(P(None, "gx", "gy", "gz"), P("gy", None, "gx", "gz")),
        check_vma=False,
    )
```

```python
import jax
import jax.numpy as jnp
from jax import lax
from jax.experimental import pallas as pl
from jax.experimental.pallas import tpu as pltpu
from jax.sharding import PartitionSpec as P

SUBSTEPS = 2
OCTET = 8
LANES = 128

flow_step = 0.15
sub_step = 0.04
smooth_eps = 1e-06


def shift(array, axis, by):
    count = lax.axis_size(axis)
    return lax.ppermute(array, axis, [(i, (i + by) % count) for i in range(count)])


def swap(array, axis, late):
    count = lax.axis_size(axis)
    pairs = [(i, (i + 1) % count) for i in range(late, count + late, 2)]
    pairs = [(a % count, b % count) for a, b in pairs]
    return lax.ppermute(array, axis, pairs + [(b, a) for a, b in pairs])


def close(array):
    return pltpu.with_memory_space_constraint(array, pltpu.VMEM)


def far(array):
    return pltpu.with_memory_space_constraint(array, pltpu.HBM)


def indicators(before, after):
    curve = after - before
    bent = 1.5 * curve
    centre = (curve * curve + 0.75 * smooth_eps) + 0.75 * (before * after)
    return centre + after * bent, centre, centre - before * bent


def faces(left, middle, right, third_low, third_high):
    ml = middle * left
    mr = middle * right
    lr = left * right
    ml = ml * ml
    mr = mr * mr
    lr = lr * lr
    total = (ml + mr) + 6.0 * lr
    first = ml * third_high
    second = mr * third_low
    both = 2.0 * (first + second)
    return (both + first) / (total + 2.0 * ml), (both + second) / (total + 2.0 * mr)


def line(load, count, speed, put):
    def kept(function):
        known = {}

        def get(i):
            if i not in known:
                known[i] = function(i)
            return known[i]

        return get

    u = kept(load)
    d = kept(lambda i: u(i + 1) - u(i))
    second = kept(lambda i: d(i) - d(i - 1))
    third = kept(lambda i: second(i) - second(i - 1))
    ind = kept(lambda i: indicators(d(i - 1), d(i)))
    both = kept(
        lambda i: faces(ind(i - 1)[0], ind(i)[1], ind(i + 1)[2], third(i), third(i + 1))
    )
    for i in range(count):
        v = speed(i)
        bend = jnp.where(
            v > 0.0,
            third(i) + (both(i)[0] - both(i - 1)[0]),
            third(i + 1) - (both(i + 1)[1] - both(i)[1]),
        )
        put(i, v * (3.0 * (d(i) + d(i - 1)) - bend))


def groups_of(species):
    return list(range(0, species - OCTET, OCTET)) + [species - OCTET]


def rounded(array):
    return array.astype(jnp.bfloat16).astype(jnp.float32)


def split_three(array):
    first = rounded(array)
    second = rounded(array - first)
    return [first, second, rounded(array - first - second)]


def prep_kernel(
    spot_ref, u_hbm, *refs,
    species, width_x, width_y, row_tiles, spans,
):
    sources, refs = refs[:7], refs[7:]
    chunk_refs, refs = refs[: len(spans)], refs[len(spans) :]
    early_ref, late_ref, zpack_ref, order_ref, net_ref, heat_ref, wind_ref, scale_ref = refs[:8]
    u_ref, zwide_ref, orders_ref, log_ref, energy_ref, net_in_ref, heat_in_ref = refs[8:15]
    sems, u_sems = refs[15:]
    pieces = u_sems.shape[0]
    bounds = [species * i // pieces for i in range(pieces + 1)]
    arrivals = [
        pltpu.make_async_copy(
            u_hbm.at[pl.ds(a, b - a)], u_ref.at[pl.ds(a, b - a)], u_sems.at[i]
        )
        for i, (a, b) in enumerate(zip(bounds, bounds[1:]))
    ]
    for copy in arrivals:
        copy.start()
    targets = (wind_ref, scale_ref, orders_ref, log_ref, energy_ref, net_in_ref, heat_in_ref)
    copies = [
        pltpu.make_async_copy(source, target, sems.at[i])
        for i, (source, target) in enumerate(zip(sources, targets))
    ]
    for copy in copies:
        copy.start()
    pencils = width_x * width_y
    for copy, a, b in zip(arrivals, bounds, bounds[1:]):
        copy.wait()
        for c, (y0, y1) in enumerate(spans):
            for x in range(width_x):
                chunk_refs[c][a:b, x] = u_ref[
                    a:b, x * width_y + y0 : x * width_y + y1, :
                ].astype(jnp.bfloat16)
    flat = u_ref.reshape(species * pencils, LANES)
    odd = lax.rem(spot_ref[0], 2)
    for g, s0 in enumerate(groups_of(species)):
        for x in range(width_x):
            for k in range(3):
                at = s0 * pencils + x * width_y + k
                shown = (x * 3 + k, slice(g * OCTET, (g + 1) * OCTET))
                early_ref[shown] = flat[
                    pl.ds(at + (1 - odd) * (width_y - 3), OCTET, stride=pencils), :
                ].astype(jnp.bfloat16)
                late_ref[shown] = flat[
                    pl.ds(at + odd * (width_y - 3), OCTET, stride=pencils), :
                ].astype(jnp.bfloat16)
    k = lax.broadcasted_iota(jnp.int32, (OCTET, LANES), 0)
    z = lax.broadcasted_iota(jnp.int32, (OCTET, LANES), 1)
    pick = jnp.where(
        ((k < 3) & (z == k)) | ((k >= 3) & (k < 6) & (z == LANES - 6 + k)), 1.0, 0.0
    ).astype(jnp.bfloat16)
    rows = species * pencils
    slots = zpack_ref.shape[0] // 6
    zwide_ref[...] = jnp.zeros(zwide_ref.shape, jnp.float32)
    for j in range(row_tiles):
        j0 = min(j * LANES, rows - LANES)
        block = flat[j0 : j0 + LANES, :].astype(jnp.bfloat16)
        ends = lax.dot_general(
            pick, block, (((1,), (1,)), ((), ())), preferred_element_type=jnp.float32
        )
        zwide_ref[pl.ds(j, OCTET, stride=slots), :] = ends
    zpack_ref[...] = zwide_ref[: 6 * slots, :].astype(jnp.bfloat16)

    for copy in copies:
        copy.wait()
    reactions, wide = order_ref.shape
    row = lax.broadcasted_iota(jnp.int32, (species, wide), 0)
    col = lax.broadcasted_iota(jnp.int32, (species, wide), 1)
    same = jnp.where(row == col, 1.0, 0.0).astype(jnp.bfloat16)
    bias = split_three(-energy_ref[...]) + split_three(log_ref[...])
    bias = jnp.concatenate(bias + [jnp.zeros((2, reactions), jnp.float32)], axis=0)
    row = lax.broadcasted_iota(jnp.int32, (OCTET, wide), 0)
    col = lax.broadcasted_iota(jnp.int32, (OCTET, wide), 1)
    late = jnp.where(col == wide - OCTET + row, 1.0, 0.0).astype(jnp.bfloat16)
    order_ref[...] = (
        lax.dot_general(
            orders_ref[...], same, (((0,), (0,)), ((), ())), preferred_element_type=jnp.float32
        )
        + lax.dot_general(
            bias.astype(jnp.bfloat16), late, (((0,), (0,)), ((), ())),
            preferred_element_type=jnp.float32,
        )
    ).astype(jnp.bfloat16)
    row = lax.broadcasted_iota(jnp.int32, (wide, species), 0)
    col = lax.broadcasted_iota(jnp.int32, (wide, species), 1)
    same = jnp.where(row == col, 1.0, 0.0).astype(jnp.bfloat16)
    net_ref[...] = jnp.dot(
        same, net_in_ref[...], preferred_element_type=jnp.float32
    ).astype(jnp.bfloat16)
    heats = split_three(-heat_in_ref[...])
    heats = jnp.concatenate(heats + [jnp.zeros((5, species), jnp.float32)], axis=0)
    heat_ref[...] = lax.dot_general(
        heats.astype(jnp.bfloat16), same, (((1,), (1,)), ((), ())),
        preferred_element_type=jnp.float32,
    ).astype(jnp.bfloat16)


def upward_kernel(
    u_ref, zlow_ref, zhigh_ref, v_ref, out_ref, across_ref, speed_ref, moved_ref,
    *, species, pencils, row_tiles, slots, pitch,
):
    rows = species * pencils
    flat = u_ref.reshape(rows, LANES)

    def first_row(j):
        return min(j * LANES, rows - LANES)

    for j in range(row_tiles, slots):
        across_ref[j * pitch : (j + 1) * pitch, :] = jnp.zeros((pitch, LANES), jnp.float32)
        speed_ref[j * pitch : (j + 1) * pitch, :] = jnp.zeros((pitch, LANES), jnp.float32)
    wind = v_ref[2]
    turned = {}
    for j in range(row_tiles):
        p0 = first_row(j) % pencils
        if p0 not in turned:
            strips, need, at = [], LANES, p0
            while need > 0:
                take = min(need, pencils - at)
                strips.append(wind[at : at + take])
                need, at = need - take, 0
            turned[p0] = jnp.concatenate(strips, axis=0).T
    for j in range(row_tiles):
        speed_ref[j * pitch : j * pitch + LANES, :] = turned[first_row(j) % pencils]
    for j in range(row_tiles):
        j0 = first_row(j)
        across_ref[j * pitch : j * pitch + LANES, :] = flat[j0 : j0 + LANES, :].T

    def upward(q, carry):
        t0 = pl.multiple_of(q * OCTET, OCTET)
        base = t0 * pitch

        def load(i):
            if i < 0:
                return zlow_ref[pl.ds((i + 6) * slots + t0, OCTET), :].astype(jnp.float32)
            if i >= LANES:
                return zhigh_ref[pl.ds((i - LANES) * slots + t0, OCTET), :].astype(jnp.float32)
            return across_ref[pl.ds(base + i, OCTET, stride=pitch), :]

        def speed(i):
            return speed_ref[pl.ds(base + i, OCTET, stride=pitch), :]

        def put(i, value):
            moved_ref[pl.ds(base + i, OCTET, stride=pitch), :] = value

        line(load, LANES, speed, put)
        return carry

    lax.fori_loop(0, slots // OCTET, upward, 0)

    for j in range(row_tiles):
        j0 = j * LANES
        size = min(LANES, rows - j0)
        skip = j0 - first_row(j)
        out_ref[j0 : j0 + size, :] = moved_ref[j * pitch : j * pitch + LANES, :].T[skip:]


def north_kernel(
    spot_ref, u_ref, early_ref, late_ref, v_ref, acc_ref,
    *, species, width_x, width_y,
):
    pencils = width_x * width_y
    rows = species * pencils
    flat = u_ref.reshape(rows, LANES)
    count = len(groups_of(species))
    odd = lax.rem(spot_ref[0], 2) == 1

    def north(step, carry):
        g = step // width_x
        x = step % width_x
        s0 = jnp.minimum(g * OCTET, species - OCTET)
        base = s0 * pencils + x * width_y
        g0 = pl.multiple_of(g * OCTET, OCTET)

        def load(i):
            if i < 0 or i >= width_y:
                at = (x * 3 + (i + 3 if i < 0 else i - width_y), pl.ds(g0, OCTET))
                ours, other = early_ref[at], late_ref[at]
                if i >= width_y:
                    ours, other = other, ours
                return jnp.where(odd, ours.astype(jnp.float32), other.astype(jnp.float32))
            return flat[pl.ds(base + i, OCTET, stride=pencils), :]

        def speed(i):
            return jnp.broadcast_to(v_ref[1, pl.ds(x * width_y + i, 1), :], (OCTET, LANES))

        def put(i, value):
            acc_ref[pl.ds(base + i, OCTET, stride=pencils), :] = value

        line(load, width_y, speed, put)
        return carry

    lax.fori_loop(0, count * width_x, north, 0)


def chunk_kernel(
    me_ref, hot_ref, u_ref, part_ref, raised_ref, early_ref, late_ref, wind_ref, scale_ref,
    order_ref, net_ref, heat_ref, basis_ref, *refs,
    species, width_x, span, members, share, first, last,
):
    refs = list(refs)
    before_ref = None
    if not first:
        before_ref = refs.pop(0)
        refs.pop(0)
    out_hbm = refs.pop(0)
    out_ref, cells_ref, out_sems = refs[-3:]
    refs = refs[:-3]
    release_ref = refs.pop() if last else refs.pop(0)
    y0, y1 = span
    width = y1 - y0
    octets = width // OCTET
    together = 2 if octets == 1 else 1
    odd = lax.rem(me_ref[0], 2)
    width_y = scale_ref.shape[1]
    u_ref = u_ref.reshape(species, width_x, width_y, LANES)
    part_ref = part_ref.reshape(species, width_x, width_y, LANES)
    raised_ref = raised_ref.reshape(species, width_x, width_y, LANES)

    def east(s, low_ref, high_ref):
        for o in range(octets):
            at = slice(o * OCTET, (o + 1) * OCTET)
            there = slice(y0 + o * OCTET, y0 + (o + 1) * OCTET)

            def load(i):
                if i < 0:
                    return low_ref[s, i + width_x, at].astype(jnp.float32)
                if i >= width_x:
                    return high_ref[s, i - width_x, at].astype(jnp.float32)
                return u_ref[s, i, there]

            def put(i, value):
                others = part_ref[s, i, there] + raised_ref[s, i, there]
                out_ref[s, i, at] = u_ref[s, i, there] - (flow_step / 6.0) * (value + others)

            line(load, width_x, lambda i: wind_ref[0, i * width_y + there.start : i * width_y + there.stop], put)

    for parity, low_ref, high_ref in ((0, late_ref, early_ref), (1, early_ref, late_ref)):

        @pl.when(odd == parity)
        def _(low_ref=low_ref, high_ref=high_ref):
            def several(step, carry):
                for extra in range(together):
                    east(step * together + extra, low_ref, high_ref)
                return carry

            lax.fori_loop(0, species // together, several, 0)
            for rest in range(species // together * together, species):
                east(rest, low_ref, high_ref)

    if first:
        release_ref[...] = jnp.zeros(release_ref.shape, jnp.float32)
    else:
        release_ref[...] = before_ref[...]
    rows = width_x * width
    flat = out_ref.reshape(species * rows, LANES)
    starts = [(s0, min(OCTET, species - s0)) for s0 in range(0, species, OCTET)]
    sublane = lax.broadcasted_iota(jnp.int32, (OCTET, LANES), 0)
    order = order_ref[...]
    net = net_ref[...]
    heat = heat_ref[...]
    depth = order.shape[1]
    for block in range(width_x * octets):
        x, o = block // octets, block % octets
        for y in range(OCTET):
            cols = slice(y * LANES, (y + 1) * LANES)
            at = x * width + o * OCTET + y
            cells_ref[block, depth - 2 * OCTET : depth - OCTET, cols] = jnp.zeros(
                (OCTET, LANES), jnp.float32
            )
            for s0, size in starts:
                cells_ref[block, s0 : s0 + size, cols] = flat[
                    pl.ds(s0 * rows + at, size, stride=rows), :
                ]
            theta = jnp.broadcast_to(
                scale_ref[x, y0 + o * OCTET + y : y0 + o * OCTET + y + 1, :], (OCTET, LANES)
            )
            cells_ref[block, depth - OCTET :, cols] = jnp.where(
                sublane < 3, theta, jnp.where(sublane < 6, 1.0, 0.0)
            )
    stores = []
    for block in range(width_x * octets):
        x, o = block // octets, block % octets
        start = rounded(cells_ref[block])
        current = start
        for _ in range(SUBSTEPS):
            features = current.astype(jnp.bfloat16)
            exponent = jnp.dot(order, features, preferred_element_type=jnp.float32)
            rates = jnp.exp(exponent).astype(jnp.bfloat16)
            source = jnp.dot(net, rates, preferred_element_type=jnp.float32)
            current = current + sub_step * rounded(source)
        increment = rounded(current - start)
        gains = []
        for y in range(OCTET):
            cols = slice(y * LANES, (y + 1) * LANES)
            row = y0 + o * OCTET + y
            at = x * width + o * OCTET + y
            gain = jnp.where(hot_ref[x, 0, row] > 0, increment[:, cols], 0.0)
            for s0, size in starts:
                flat[pl.ds(s0 * rows + at, size, stride=rows), :] = (
                    cells_ref[block, s0 : s0 + size, cols] + gain[s0 : s0 + size, :]
                )
            gains.append(gain.astype(jnp.bfloat16))
        sums = jnp.dot(
            heat, jnp.concatenate(gains, axis=1), preferred_element_type=jnp.float32
        )
        sums = sums[0:1] + sums[1:2] + sums[2:3]
        for y in range(OCTET):
            row = y0 + o * OCTET + y
            release_ref[row // share, x, row % share : row % share + 1, :] = sums[
                :, y * LANES : (y + 1) * LANES
            ]
        if o == octets - 1:
            stores.append(
                pltpu.make_async_copy(
                    out_ref.at[:, x], out_hbm.at[:, x, pl.ds(y0, width)], out_sems.at[x]
                )
            )
            stores[-1].start()
    if last:
        modes = basis_ref.shape[1]
        for k in range(members):
            for x in range(width_x):
                release_ref[k, x, OCTET - 1 :, 0:modes] = basis_ref[x : x + 1, :]
        for j in range(members):
            refs[j][...] = release_ref[lax.rem(me_ref[0] + j, members)]
    for store in stores:
        store.wait()


def core_kernel(*refs, members, width_x, share, modes):
    parts = refs[:members]
    out_ref, rows_ref = refs[members:]
    lines = members * width_x
    padded = rows_ref.shape[0] // OCTET
    for j in range(members):
        for x in range(width_x):
            at = (j * width_x + x) * OCTET
            rows_ref[at : at + OCTET, :] = parts[j][x]
    if padded > lines:
        rows_ref[lines * OCTET :, :] = jnp.zeros(((padded - lines) * OCTET, LANES), jnp.float32)

    def gather(y):
        return jnp.concatenate(
            [
                rows_ref[pl.ds(a * OCTET * OCTET + y, OCTET, stride=OCTET), :]
                for a in range(padded // OCTET)
            ],
            axis=0,
        )

    basis = gather(OCTET - 1).T[:modes]
    for y in range(share):
        out_ref[y] = jnp.dot(
            basis, gather(y), preferred_element_type=jnp.float32, precision=lax.Precision.HIGHEST
        )


def body(
    chemical_log_concentrations,
    advection_wind,
    inverse_thermal_scale,
    kinetics_column_switch,
    kinetic_exponents,
    arrhenius_log_coefficient,
    arrhenius_energy,
    stoichiometric_production,
    formation_heat,
    streamwise_tucker_basis,
):
    species, width_x, width_y, depth = chemical_log_concentrations.shape
    pencils = width_x * width_y
    rows = species * pencils
    row_tiles = -(-rows // LANES)
    slots = -(-row_tiles // OCTET) * OCTET
    pitch = LANES + OCTET
    padded = len(groups_of(species)) * OCTET
    reactions = kinetic_exponents.shape[0]
    members = lax.axis_size("gx")
    share = width_y // members
    modes = streamwise_tucker_basis.shape[1]
    cut = width_y - OCTET
    spans = [(0, cut), (cut, width_y)]
    vmem = pl.BlockSpec(memory_space=pltpu.VMEM)
    smem = pl.BlockSpec(memory_space=pltpu.SMEM)
    flat_source = chemical_log_concentrations.reshape(species, pencils, depth)
    params = pltpu.CompilerParams(vmem_limit_bytes=32 * 1024 * 1024)

    def chunk(span):
        return jax.ShapeDtypeStruct((species, width_x, span[1] - span[0], LANES), jnp.bfloat16)

    side = jax.ShapeDtypeStruct((width_x * 3, padded, LANES), jnp.bfloat16)
    any_spec = pl.BlockSpec(memory_space=pl.ANY)
    me = lax.axis_index("gx").astype(jnp.int32).reshape(1)
    spot = lax.axis_index("gy").astype(jnp.int32).reshape(1)
    *chunks, y_early, y_late, z_own, order, net, heat, wind, scale, flat_u = pl.pallas_call(
        lambda *refs: prep_kernel(
            *refs, species=species, width_x=width_x, width_y=width_y, row_tiles=row_tiles,
            spans=spans,
        ),
        in_specs=[smem] + [any_spec] * 8,
        out_specs=[vmem] * (len(spans) + 9),
        out_shape=[chunk(span) for span in spans]
        + [
            side,
            side,
            jax.ShapeDtypeStruct((6 * slots, LANES), jnp.bfloat16),
            jax.ShapeDtypeStruct((reactions, padded + OCTET), jnp.bfloat16),
            jax.ShapeDtypeStruct((padded + OCTET, reactions), jnp.bfloat16),
            jax.ShapeDtypeStruct((OCTET, padded + OCTET), jnp.bfloat16),
            pltpu.VMEM((3, pencils, depth), jnp.float32),
            pltpu.VMEM((width_x, width_y, depth), jnp.float32),
            pltpu.VMEM((species, pencils, depth), jnp.float32),
        ],
        scratch_shapes=[
            pltpu.VMEM((OCTET * slots, LANES), jnp.float32),
            pltpu.VMEM((species, reactions), jnp.bfloat16),
            pltpu.VMEM((1, reactions), jnp.float32),
            pltpu.VMEM((1, reactions), jnp.float32),
            pltpu.VMEM((species, reactions), jnp.bfloat16),
            pltpu.VMEM((1, species), jnp.float32),
            pltpu.SemaphoreType.DMA((7,)),
            pltpu.SemaphoreType.DMA((4,)),
        ],
        compiler_params=params,
        name="prep",
    )(
        spot,
        far(flat_source),
        far(advection_wind.reshape(3, pencils, depth)),
        far(inverse_thermal_scale),
        far(kinetic_exponents.T),
        far(arrhenius_log_coefficient.reshape(1, reactions)),
        far(arrhenius_energy.reshape(1, reactions)),
        far(stoichiometric_production),
        far(formation_heat.reshape(1, species)),
    )

    z_low = shift(z_own, "gz", 1)
    z_high = z_low if lax.axis_size("gz") == 2 else shift(z_own, "gz", -1)
    x_late = [swap(chunks[0], "gx", 1)]
    late_rows = swap(y_late, "gy", 1)
    early_rows = swap(y_early, "gy", 0)
    x_early = [swap(part, "gx", 0) for part in chunks]
    x_late += [swap(part, "gx", 1) for part in chunks[1:]]

    cells = rows * depth
    raised = pl.pallas_call(
        lambda *refs: upward_kernel(
            *refs, species=species, pencils=pencils, row_tiles=row_tiles, slots=slots, pitch=pitch
        ),
        in_specs=[vmem] * 4,
        out_specs=vmem,
        out_shape=pltpu.VMEM((rows, depth), jnp.float32),
        scratch_shapes=[pltpu.VMEM((slots * pitch, LANES), jnp.float32)] * 3,
        cost_estimate=pl.CostEstimate(
            flops=cells * 60, bytes_accessed=cells * 8, transcendentals=cells * 2
        ),
        compiler_params=params,
        name="upward",
    )(flat_u, close(z_low), close(z_high), wind)
    part = pl.pallas_call(
        lambda *refs: north_kernel(*refs, species=species, width_x=width_x, width_y=width_y),
        in_specs=[smem] + [vmem] * 4,
        out_specs=vmem,
        out_shape=pltpu.VMEM((rows, depth), jnp.float32),
        cost_estimate=pl.CostEstimate(
            flops=cells * 60, bytes_accessed=cells * 8, transcendentals=cells * 2
        ),
        compiler_params=params,
        name="north",
    )(spot, flat_u, close(early_rows), close(late_rows), wind)
    state = None

    hot = jnp.swapaxes(kinetics_column_switch, 2, 3).reshape(width_x, 1, width_y)
    release = None
    tile = jax.ShapeDtypeStruct((width_x, OCTET, LANES), jnp.float32)
    pile = jax.ShapeDtypeStruct((members, width_x, OCTET, LANES), jnp.float32)
    for c, span in enumerate(spans):
        width = span[1] - span[0]
        first, last = c == 0, c == len(spans) - 1

        outs = [tile] * members if last else [pile]
        results = pl.pallas_call(
            lambda *refs, first=first, last=last, span=span: chunk_kernel(
                *refs, species=species, width_x=width_x, span=span, members=members,
                share=share, first=first, last=last,
            ),
            in_specs=[smem, smem] + [vmem] * 11 + ([] if first else [vmem, any_spec]),
            out_specs=[any_spec] + [vmem] * len(outs),
            out_shape=[jax.ShapeDtypeStruct(chemical_log_concentrations.shape, jnp.float32)] + outs,
            scratch_shapes=([pltpu.VMEM(pile.shape, jnp.float32)] if last else [])
            + [
                pltpu.VMEM((species, width_x, width, LANES), jnp.float32),
                pltpu.VMEM(
                    (width_x * width // OCTET, padded + OCTET, OCTET * LANES), jnp.float32
                ),
                pltpu.SemaphoreType.DMA((width_x,)),
            ],
            input_output_aliases={} if first else {14: 0},
            compiler_params=pltpu.CompilerParams(vmem_limit_bytes=32 * 1024 * 1024),
            cost_estimate=pl.CostEstimate(
                flops=cells * 60, bytes_accessed=cells * 4, transcendentals=cells * 4
            ),
        )(
            me, hot, flat_u, part, raised, close(x_early[c]), close(x_late[c]), wind, scale, order, net, heat, streamwise_tucker_basis,
            *([] if first else [release, state]),
        )
        state = results[0]
        release = results[1]
    pieces = results[1:]

    moved = [pieces[0]] + [close(shift(pieces[j], "gx", j)) for j in range(1, members)]
    lines = -(-members * width_x // OCTET) * OCTET
    core = pl.pallas_call(
        lambda *refs: core_kernel(
            *refs, members=members, width_x=width_x, share=share, modes=modes
        ),
        in_specs=[vmem] * members,
        out_specs=vmem,
        out_shape=jax.ShapeDtypeStruct((share, modes, depth), jnp.float32),
        scratch_shapes=[pltpu.VMEM((lines * OCTET, LANES), jnp.float32)],
        compiler_params=params,
        name="core",
    )(*moved)
    return (state, core.transpose(1, 0, 2)[None])


def solution(mesh):
    placed = (
        P(None, "gx", "gy", "gz"),
        P(None, "gx", "gy", "gz"),
        P("gx", "gy", "gz"),
        P(None, "gx", "gy", "gz"),
        P(),
        P(),
        P(),
        P(),
        P(),
        P("gx", None),
    )
    return jax.shard_map(
        body,
        mesh=mesh,
        in_specs=placed,
        out_specs=(P(None, "gx", "gy", "gz"), P("gy", None, "gx", "gz")),
        check_vma=False,
    )
```

```python
import jax
import jax.numpy as jnp
from jax import lax
from jax.experimental import pallas as pl
from jax.experimental.pallas import tpu as pltpu
from jax.sharding import PartitionSpec as P

SUBSTEPS = 2
OCTET = 8
LANES = 128

flow_step = 0.15
sub_step = 0.04
smooth_eps = 1e-06


def shift(array, axis, by):
    count = lax.axis_size(axis)
    return lax.ppermute(array, axis, [(i, (i + by) % count) for i in range(count)])


def swap(array, axis, late):
    count = lax.axis_size(axis)
    pairs = [(i, (i + 1) % count) for i in range(late, count + late, 2)]
    pairs = [(a % count, b % count) for a, b in pairs]
    return lax.ppermute(array, axis, pairs + [(b, a) for a, b in pairs])


def close(array):
    return pltpu.with_memory_space_constraint(array, pltpu.VMEM)


def far(array):
    return pltpu.with_memory_space_constraint(array, pltpu.HBM)


def indicators(before, after):
    curve = after - before
    bent = 1.5 * curve
    centre = (curve * curve + 0.75 * smooth_eps) + 0.75 * (before * after)
    return centre + after * bent, centre, centre - before * bent


def faces(left, middle, right, third_low, third_high):
    ml = middle * left
    mr = middle * right
    lr = left * right
    ml = ml * ml
    mr = mr * mr
    lr = lr * lr
    total = (ml + mr) + 6.0 * lr
    first = ml * third_high
    second = mr * third_low
    both = 2.0 * (first + second)
    return (both + first) / (total + 2.0 * ml), (both + second) / (total + 2.0 * mr)


def line(load, count, speed, put):
    def kept(function):
        known = {}

        def get(i):
            if i not in known:
                known[i] = function(i)
            return known[i]

        return get

    u = kept(load)
    d = kept(lambda i: u(i + 1) - u(i))
    second = kept(lambda i: d(i) - d(i - 1))
    third = kept(lambda i: second(i) - second(i - 1))
    ind = kept(lambda i: indicators(d(i - 1), d(i)))
    both = kept(
        lambda i: faces(ind(i - 1)[0], ind(i)[1], ind(i + 1)[2], third(i), third(i + 1))
    )
    for i in range(count):
        v = speed(i)
        bend = jnp.where(
            v > 0.0,
            third(i) + (both(i)[0] - both(i - 1)[0]),
            third(i + 1) - (both(i + 1)[1] - both(i)[1]),
        )
        put(i, v * (3.0 * (d(i) + d(i - 1)) - bend))


def groups_of(species):
    return list(range(0, species - OCTET, OCTET)) + [species - OCTET]


def rounded(array):
    return array.astype(jnp.bfloat16).astype(jnp.float32)


def split_three(array):
    first = rounded(array)
    second = rounded(array - first)
    return [first, second, rounded(array - first - second)]


def prep_kernel(
    spot_ref, u_hbm, *refs,
    species, width_x, width_y, row_tiles, spans,
):
    sources, refs = refs[:7], refs[7:]
    chunk_refs, refs = refs[: len(spans)], refs[len(spans) :]
    early_ref, late_ref, zpack_ref, order_ref, net_ref, heat_ref, wind_ref, scale_ref = refs[:8]
    u_ref, zwide_ref, orders_ref, log_ref, energy_ref, net_in_ref, heat_in_ref = refs[8:15]
    sems, u_sems = refs[15:]
    pieces = u_sems.shape[0]
    bounds = [species * i // pieces for i in range(pieces + 1)]
    arrivals = [
        pltpu.make_async_copy(
            u_hbm.at[pl.ds(a, b - a)], u_ref.at[pl.ds(a, b - a)], u_sems.at[i]
        )
        for i, (a, b) in enumerate(zip(bounds, bounds[1:]))
    ]
    for copy in arrivals:
        copy.start()
    targets = (wind_ref, scale_ref, orders_ref, log_ref, energy_ref, net_in_ref, heat_in_ref)
    copies = [
        pltpu.make_async_copy(source, target, sems.at[i])
        for i, (source, target) in enumerate(zip(sources, targets))
    ]
    for copy in copies:
        copy.start()
    pencils = width_x * width_y
    for copy, a, b in zip(arrivals, bounds, bounds[1:]):
        copy.wait()
        for c, (y0, y1) in enumerate(spans):
            for x in range(width_x):
                chunk_refs[c][a:b, x] = u_ref[
                    a:b, x * width_y + y0 : x * width_y + y1, :
                ].astype(jnp.bfloat16)
    flat = u_ref.reshape(species * pencils, LANES)
    odd = lax.rem(spot_ref[0], 2)
    for g, s0 in enumerate(groups_of(species)):
        for x in range(width_x):
            for k in range(3):
                at = s0 * pencils + x * width_y + k
                shown = (x * 3 + k, slice(g * OCTET, (g + 1) * OCTET))
                early_ref[shown] = flat[
                    pl.ds(at + (1 - odd) * (width_y - 3), OCTET, stride=pencils), :
                ].astype(jnp.bfloat16)
                late_ref[shown] = flat[
                    pl.ds(at + odd * (width_y - 3), OCTET, stride=pencils), :
                ].astype(jnp.bfloat16)
    k = lax.broadcasted_iota(jnp.int32, (OCTET, LANES), 0)
    z = lax.broadcasted_iota(jnp.int32, (OCTET, LANES), 1)
    pick = jnp.where(
        ((k < 3) & (z == k)) | ((k >= 3) & (k < 6) & (z == LANES - 6 + k)), 1.0, 0.0
    ).astype(jnp.bfloat16)
    rows = species * pencils
    slots = zpack_ref.shape[0] // 6
    zwide_ref[...] = jnp.zeros(zwide_ref.shape, jnp.float32)
    for j in range(row_tiles):
        j0 = min(j * LANES, rows - LANES)
        block = flat[j0 : j0 + LANES, :].astype(jnp.bfloat16)
        ends = lax.dot_general(
            pick, block, (((1,), (1,)), ((), ())), preferred_element_type=jnp.float32
        )
        zwide_ref[pl.ds(j, OCTET, stride=slots), :] = ends
    zpack_ref[...] = zwide_ref[: 6 * slots, :].astype(jnp.bfloat16)

    for copy in copies:
        copy.wait()
    reactions, wide = order_ref.shape
    row = lax.broadcasted_iota(jnp.int32, (species, wide), 0)
    col = lax.broadcasted_iota(jnp.int32, (species, wide), 1)
    same = jnp.where(row == col, 1.0, 0.0).astype(jnp.bfloat16)
    bias = split_three(-energy_ref[...]) + split_three(log_ref[...])
    bias = jnp.concatenate(bias + [jnp.zeros((2, reactions), jnp.float32)], axis=0)
    row = lax.broadcasted_iota(jnp.int32, (OCTET, wide), 0)
    col = lax.broadcasted_iota(jnp.int32, (OCTET, wide), 1)
    late = jnp.where(col == wide - OCTET + row, 1.0, 0.0).astype(jnp.bfloat16)
    order_ref[...] = (
        lax.dot_general(
            orders_ref[...], same, (((0,), (0,)), ((), ())), preferred_element_type=jnp.float32
        )
        + lax.dot_general(
            bias.astype(jnp.bfloat16), late, (((0,), (0,)), ((), ())),
            preferred_element_type=jnp.float32,
        )
    ).astype(jnp.bfloat16)
    row = lax.broadcasted_iota(jnp.int32, (wide, species), 0)
    col = lax.broadcasted_iota(jnp.int32, (wide, species), 1)
    same = jnp.where(row == col, 1.0, 0.0).astype(jnp.bfloat16)
    net_ref[...] = jnp.dot(
        same, net_in_ref[...], preferred_element_type=jnp.float32
    ).astype(jnp.bfloat16)
    heats = split_three(-heat_in_ref[...])
    heats = jnp.concatenate(heats + [jnp.zeros((5, species), jnp.float32)], axis=0)
    heat_ref[...] = lax.dot_general(
        heats.astype(jnp.bfloat16), same, (((1,), (1,)), ((), ())),
        preferred_element_type=jnp.float32,
    ).astype(jnp.bfloat16)


def upward_kernel(
    u_ref, zlow_ref, zhigh_ref, v_ref, out_ref, across_ref, speed_ref, moved_ref,
    *, species, pencils, row_tiles, slots, pitch,
):
    rows = species * pencils
    flat = u_ref.reshape(rows, LANES)

    def first_row(j):
        return min(j * LANES, rows - LANES)

    for j in range(row_tiles, slots):
        across_ref[j * pitch : (j + 1) * pitch, :] = jnp.zeros((pitch, LANES), jnp.float32)
        speed_ref[j * pitch : (j + 1) * pitch, :] = jnp.zeros((pitch, LANES), jnp.float32)
    wind = v_ref[2]
    turned = {}
    for j in range(row_tiles):
        p0 = first_row(j) % pencils
        if p0 not in turned:
            strips, need, at = [], LANES, p0
            while need > 0:
                take = min(need, pencils - at)
                strips.append(wind[at : at + take])
                need, at = need - take, 0
            turned[p0] = jnp.concatenate(strips, axis=0).T
    for j in range(row_tiles):
        speed_ref[j * pitch : j * pitch + LANES, :] = turned[first_row(j) % pencils]
    for j in range(row_tiles):
        j0 = first_row(j)
        across_ref[j * pitch : j * pitch + LANES, :] = flat[j0 : j0 + LANES, :].T

    def upward(q, carry):
        t0 = pl.multiple_of(q * OCTET, OCTET)
        base = t0 * pitch

        def load(i):
            if i < 0:
                return zlow_ref[pl.ds((i + 6) * slots + t0, OCTET), :].astype(jnp.float32)
            if i >= LANES:
                return zhigh_ref[pl.ds((i - LANES) * slots + t0, OCTET), :].astype(jnp.float32)
            return across_ref[pl.ds(base + i, OCTET, stride=pitch), :]

        def speed(i):
            return speed_ref[pl.ds(base + i, OCTET, stride=pitch), :]

        def put(i, value):
            moved_ref[pl.ds(base + i, OCTET, stride=pitch), :] = value

        line(load, LANES, speed, put)
        return carry

    lax.fori_loop(0, slots // OCTET, upward, 0)

    for j in range(row_tiles):
        j0 = j * LANES
        size = min(LANES, rows - j0)
        skip = j0 - first_row(j)
        out_ref[j0 : j0 + size, :] = moved_ref[j * pitch : j * pitch + LANES, :].T[skip:]


def north_kernel(
    spot_ref, u_ref, early_ref, late_ref, v_ref, acc_ref,
    *, species, width_x, width_y,
):
    pencils = width_x * width_y
    rows = species * pencils
    flat = u_ref.reshape(rows, LANES)
    count = len(groups_of(species))
    odd = lax.rem(spot_ref[0], 2) == 1

    def north(step, carry):
        g = step // width_x
        x = step % width_x
        s0 = jnp.minimum(g * OCTET, species - OCTET)
        base = s0 * pencils + x * width_y
        g0 = pl.multiple_of(g * OCTET, OCTET)

        def load(i):
            if i < 0 or i >= width_y:
                at = (x * 3 + (i + 3 if i < 0 else i - width_y), pl.ds(g0, OCTET))
                ours, other = early_ref[at], late_ref[at]
                if i >= width_y:
                    ours, other = other, ours
                return jnp.where(odd, ours.astype(jnp.float32), other.astype(jnp.float32))
            return flat[pl.ds(base + i, OCTET, stride=pencils), :]

        def speed(i):
            return jnp.broadcast_to(v_ref[1, pl.ds(x * width_y + i, 1), :], (OCTET, LANES))

        def put(i, value):
            acc_ref[pl.ds(base + i, OCTET, stride=pencils), :] = value

        line(load, width_y, speed, put)
        return carry

    lax.fori_loop(0, count * width_x, north, 0)


def chunk_kernel(
    me_ref, hot_ref, u_ref, part_ref, raised_ref, early_ref, late_ref, wind_ref, scale_ref,
    order_ref, net_ref, heat_ref, basis_ref, *refs,
    species, width_x, span, members, share, first, last,
):
    refs = list(refs)
    before_ref = None
    if not first:
        before_ref = refs.pop(0)
        refs.pop(0)
    out_hbm = refs.pop(0)
    out_ref, cells_ref, out_sems = refs[-3:]
    refs = refs[:-3]
    release_ref = refs.pop() if last else refs.pop(0)
    y0, y1 = span
    width = y1 - y0
    octets = width // OCTET
    together = 2 if octets == 1 else 1
    odd = lax.rem(me_ref[0], 2)
    width_y = scale_ref.shape[1]
    u_ref = u_ref.reshape(species, width_x, width_y, LANES)
    part_ref = part_ref.reshape(species, width_x, width_y, LANES)
    raised_ref = raised_ref.reshape(species, width_x, width_y, LANES)

    def east(s, low_ref, high_ref):
        for o in range(octets):
            at = slice(o * OCTET, (o + 1) * OCTET)
            there = slice(y0 + o * OCTET, y0 + (o + 1) * OCTET)

            def load(i):
                if i < 0:
                    return low_ref[s, i + width_x, at].astype(jnp.float32)
                if i >= width_x:
                    return high_ref[s, i - width_x, at].astype(jnp.float32)
                return u_ref[s, i, there]

            def put(i, value):
                others = part_ref[s, i, there] + raised_ref[s, i, there]
                out_ref[s, i, at] = u_ref[s, i, there] - (flow_step / 6.0) * (value + others)

            line(load, width_x, lambda i: wind_ref[0, i * width_y + there.start : i * width_y + there.stop], put)

    for parity, low_ref, high_ref in ((0, late_ref, early_ref), (1, early_ref, late_ref)):

        @pl.when(odd == parity)
        def _(low_ref=low_ref, high_ref=high_ref):
            def several(step, carry):
                for extra in range(together):
                    east(step * together + extra, low_ref, high_ref)
                return carry

            lax.fori_loop(0, species // together, several, 0)
            for rest in range(species // together * together, species):
                east(rest, low_ref, high_ref)

    if first:
        release_ref[...] = jnp.zeros(release_ref.shape, jnp.float32)
    else:
        release_ref[...] = before_ref[...]
    rows = width_x * width
    flat = out_ref.reshape(species * rows, LANES)
    starts = [(s0, min(OCTET, species - s0)) for s0 in range(0, species, OCTET)]
    sublane = lax.broadcasted_iota(jnp.int32, (OCTET, LANES), 0)
    order = order_ref[...]
    net = net_ref[...]
    heat = heat_ref[...]
    depth = order.shape[1]
    for block in range(width_x * octets):
        x, o = block // octets, block % octets
        for y in range(OCTET):
            cols = slice(y * LANES, (y + 1) * LANES)
            at = x * width + o * OCTET + y
            cells_ref[block, depth - 2 * OCTET : depth - OCTET, cols] = jnp.zeros(
                (OCTET, LANES), jnp.float32
            )
            for s0, size in starts:
                cells_ref[block, s0 : s0 + size, cols] = flat[
                    pl.ds(s0 * rows + at, size, stride=rows), :
                ]
            theta = jnp.broadcast_to(
                scale_ref[x, y0 + o * OCTET + y : y0 + o * OCTET + y + 1, :], (OCTET, LANES)
            )
            cells_ref[block, depth - OCTET :, cols] = jnp.where(
                sublane < 3, theta, jnp.where(sublane < 6, 1.0, 0.0)
            )
    stores = []
    blocks = range(width_x * octets)
    begun = [rounded(cells_ref[block]) for block in blocks]
    reached = list(begun)
    for _ in range(SUBSTEPS):
        for block in blocks:
            exponent = jnp.dot(
                order, reached[block].astype(jnp.bfloat16), preferred_element_type=jnp.float32
            )
            rates = jnp.exp(exponent).astype(jnp.bfloat16)
            source = jnp.dot(net, rates, preferred_element_type=jnp.float32)
            reached[block] = reached[block] + sub_step * rounded(source)
    for block in blocks:
        x, o = block // octets, block % octets
        start, current = begun[block], reached[block]
        increment = rounded(current - start)
        gains = []
        for y in range(OCTET):
            cols = slice(y * LANES, (y + 1) * LANES)
            row = y0 + o * OCTET + y
            at = x * width + o * OCTET + y
            gain = jnp.where(hot_ref[x, 0, row] > 0, increment[:, cols], 0.0)
            for s0, size in starts:
                flat[pl.ds(s0 * rows + at, size, stride=rows), :] = (
                    cells_ref[block, s0 : s0 + size, cols] + gain[s0 : s0 + size, :]
                )
            gains.append(gain.astype(jnp.bfloat16))
        sums = jnp.dot(
            heat, jnp.concatenate(gains, axis=1), preferred_element_type=jnp.float32
        )
        sums = sums[0:1] + sums[1:2] + sums[2:3]
        for y in range(OCTET):
            row = y0 + o * OCTET + y
            release_ref[row // share, x, row % share : row % share + 1, :] = sums[
                :, y * LANES : (y + 1) * LANES
            ]
        if o == octets - 1:
            stores.append(
                pltpu.make_async_copy(
                    out_ref.at[:, x], out_hbm.at[:, x, pl.ds(y0, width)], out_sems.at[x]
                )
            )
            stores[-1].start()
    if last:
        modes = basis_ref.shape[1]
        for k in range(members):
            for x in range(width_x):
                release_ref[k, x, OCTET - 1 :, 0:modes] = basis_ref[x : x + 1, :]
        for j in range(members):
            refs[j][...] = release_ref[lax.rem(me_ref[0] + j, members)]
    for store in stores:
        store.wait()


def core_kernel(*refs, members, width_x, share, modes):
    parts = refs[:members]
    out_ref, rows_ref = refs[members:]
    lines = members * width_x
    padded = rows_ref.shape[0] // OCTET
    for j in range(members):
        for x in range(width_x):
            at = (j * width_x + x) * OCTET
            rows_ref[at : at + OCTET, :] = parts[j][x]
    if padded > lines:
        rows_ref[lines * OCTET :, :] = jnp.zeros(((padded - lines) * OCTET, LANES), jnp.float32)

    def gather(y):
        return jnp.concatenate(
            [
                rows_ref[pl.ds(a * OCTET * OCTET + y, OCTET, stride=OCTET), :]
                for a in range(padded // OCTET)
            ],
            axis=0,
        )

    basis = gather(OCTET - 1).T[:modes]
    for y in range(share):
        out_ref[y] = jnp.dot(
            basis, gather(y), preferred_element_type=jnp.float32, precision=lax.Precision.HIGHEST
        )


def body(
    chemical_log_concentrations,
    advection_wind,
    inverse_thermal_scale,
    kinetics_column_switch,
    kinetic_exponents,
    arrhenius_log_coefficient,
    arrhenius_energy,
    stoichiometric_production,
    formation_heat,
    streamwise_tucker_basis,
):
    species, width_x, width_y, depth = chemical_log_concentrations.shape
    pencils = width_x * width_y
    rows = species * pencils
    row_tiles = -(-rows // LANES)
    slots = -(-row_tiles // OCTET) * OCTET
    pitch = LANES + OCTET
    padded = len(groups_of(species)) * OCTET
    reactions = kinetic_exponents.shape[0]
    members = lax.axis_size("gx")
    share = width_y // members
    modes = streamwise_tucker_basis.shape[1]
    cut = width_y - OCTET
    spans = [(0, cut), (cut, width_y)]
    vmem = pl.BlockSpec(memory_space=pltpu.VMEM)
    smem = pl.BlockSpec(memory_space=pltpu.SMEM)
    flat_source = chemical_log_concentrations.reshape(species, pencils, depth)
    params = pltpu.CompilerParams(vmem_limit_bytes=32 * 1024 * 1024)

    def chunk(span):
        return jax.ShapeDtypeStruct((species, width_x, span[1] - span[0], LANES), jnp.bfloat16)

    side = jax.ShapeDtypeStruct((width_x * 3, padded, LANES), jnp.bfloat16)
    any_spec = pl.BlockSpec(memory_space=pl.ANY)
    me = lax.axis_index("gx").astype(jnp.int32).reshape(1)
    spot = lax.axis_index("gy").astype(jnp.int32).reshape(1)
    *chunks, y_early, y_late, z_own, order, net, heat, wind, scale, flat_u = pl.pallas_call(
        lambda *refs: prep_kernel(
            *refs, species=species, width_x=width_x, width_y=width_y, row_tiles=row_tiles,
            spans=spans,
        ),
        in_specs=[smem] + [any_spec] * 8,
        out_specs=[vmem] * (len(spans) + 9),
        out_shape=[chunk(span) for span in spans]
        + [
            side,
            side,
            jax.ShapeDtypeStruct((6 * slots, LANES), jnp.bfloat16),
            jax.ShapeDtypeStruct((reactions, padded + OCTET), jnp.bfloat16),
            jax.ShapeDtypeStruct((padded + OCTET, reactions), jnp.bfloat16),
            jax.ShapeDtypeStruct((OCTET, padded + OCTET), jnp.bfloat16),
            pltpu.VMEM((3, pencils, depth), jnp.float32),
            pltpu.VMEM((width_x, width_y, depth), jnp.float32),
            pltpu.VMEM((species, pencils, depth), jnp.float32),
        ],
        scratch_shapes=[
            pltpu.VMEM((OCTET * slots, LANES), jnp.float32),
            pltpu.VMEM((species, reactions), jnp.bfloat16),
            pltpu.VMEM((1, reactions), jnp.float32),
            pltpu.VMEM((1, reactions), jnp.float32),
            pltpu.VMEM((species, reactions), jnp.bfloat16),
            pltpu.VMEM((1, species), jnp.float32),
            pltpu.SemaphoreType.DMA((7,)),
            pltpu.SemaphoreType.DMA((4,)),
        ],
        compiler_params=params,
        name="prep",
    )(
        spot,
        far(flat_source),
        far(advection_wind.reshape(3, pencils, depth)),
        far(inverse_thermal_scale),
        far(kinetic_exponents.T),
        far(arrhenius_log_coefficient.reshape(1, reactions)),
        far(arrhenius_energy.reshape(1, reactions)),
        far(stoichiometric_production),
        far(formation_heat.reshape(1, species)),
    )

    z_low = shift(z_own, "gz", 1)
    z_high = z_low if lax.axis_size("gz") == 2 else shift(z_own, "gz", -1)
    x_late = [swap(chunks[0], "gx", 1)]
    late_rows = swap(y_late, "gy", 1)
    early_rows = swap(y_early, "gy", 0)
    x_early = [swap(part, "gx", 0) for part in chunks]
    x_late += [swap(part, "gx", 1) for part in chunks[1:]]

    cells = rows * depth
    raised = pl.pallas_call(
        lambda *refs: upward_kernel(
            *refs, species=species, pencils=pencils, row_tiles=row_tiles, slots=slots, pitch=pitch
        ),
        in_specs=[vmem] * 4,
        out_specs=vmem,
        out_shape=pltpu.VMEM((rows, depth), jnp.float32),
        scratch_shapes=[pltpu.VMEM((slots * pitch, LANES), jnp.float32)] * 3,
        cost_estimate=pl.CostEstimate(
            flops=cells * 60, bytes_accessed=cells * 8, transcendentals=cells * 2
        ),
        compiler_params=params,
        name="upward",
    )(flat_u, close(z_low), close(z_high), wind)
    part = pl.pallas_call(
        lambda *refs: north_kernel(*refs, species=species, width_x=width_x, width_y=width_y),
        in_specs=[smem] + [vmem] * 4,
        out_specs=vmem,
        out_shape=pltpu.VMEM((rows, depth), jnp.float32),
        cost_estimate=pl.CostEstimate(
            flops=cells * 60, bytes_accessed=cells * 8, transcendentals=cells * 2
        ),
        compiler_params=params,
        name="north",
    )(spot, flat_u, close(early_rows), close(late_rows), wind)
    state = None

    hot = jnp.swapaxes(kinetics_column_switch, 2, 3).reshape(width_x, 1, width_y)
    release = None
    tile = jax.ShapeDtypeStruct((width_x, OCTET, LANES), jnp.float32)
    pile = jax.ShapeDtypeStruct((members, width_x, OCTET, LANES), jnp.float32)
    for c, span in enumerate(spans):
        width = span[1] - span[0]
        first, last = c == 0, c == len(spans) - 1

        outs = [tile] * members if last else [pile]
        results = pl.pallas_call(
            lambda *refs, first=first, last=last, span=span: chunk_kernel(
                *refs, species=species, width_x=width_x, span=span, members=members,
                share=share, first=first, last=last,
            ),
            in_specs=[smem, smem] + [vmem] * 11 + ([] if first else [vmem, any_spec]),
            out_specs=[any_spec] + [vmem] * len(outs),
            out_shape=[jax.ShapeDtypeStruct(chemical_log_concentrations.shape, jnp.float32)] + outs,
            scratch_shapes=([pltpu.VMEM(pile.shape, jnp.float32)] if last else [])
            + [
                pltpu.VMEM((species, width_x, width, LANES), jnp.float32),
                pltpu.VMEM(
                    (width_x * width // OCTET, padded + OCTET, OCTET * LANES), jnp.float32
                ),
                pltpu.SemaphoreType.DMA((width_x,)),
            ],
            input_output_aliases={} if first else {14: 0},
            compiler_params=pltpu.CompilerParams(vmem_limit_bytes=32 * 1024 * 1024),
            cost_estimate=pl.CostEstimate(
                flops=cells * 60, bytes_accessed=cells * 4, transcendentals=cells * 4
            ),
        )(
            me, hot, flat_u, part, raised, close(x_early[c]), close(x_late[c]), wind, scale, order, net, heat, streamwise_tucker_basis,
            *([] if first else [release, state]),
        )
        state = results[0]
        release = results[1]
    pieces = results[1:]

    moved = [pieces[0]] + [close(shift(pieces[j], "gx", j)) for j in range(1, members)]
    lines = -(-members * width_x // OCTET) * OCTET
    core = pl.pallas_call(
        lambda *refs: core_kernel(
            *refs, members=members, width_x=width_x, share=share, modes=modes
        ),
        in_specs=[vmem] * members,
        out_specs=vmem,
        out_shape=jax.ShapeDtypeStruct((share, modes, depth), jnp.float32),
        scratch_shapes=[pltpu.VMEM((lines * OCTET, LANES), jnp.float32)],
        compiler_params=params,
        name="core",
    )(*moved)
    return (state, core.transpose(1, 0, 2)[None])


def solution(mesh):
    placed = (
        P(None, "gx", "gy", "gz"),
        P(None, "gx", "gy", "gz"),
        P("gx", "gy", "gz"),
        P(None, "gx", "gy", "gz"),
        P(),
        P(),
        P(),
        P(),
        P(),
        P("gx", None),
    )
    return jax.shard_map(
        body,
        mesh=mesh,
        in_specs=placed,
        out_specs=(P(None, "gx", "gy", "gz"), P("gy", None, "gx", "gz")),
        check_vma=False,
    )
```
